32 devices in a mesh: dp: 8 (over y, x, core), tensor: 4 (over z).
Axes of the slice: x: 2, y: 2, z: 4, core: 2. Of those that a mesh axis runs over, the one named last changes fastest.
Arguments:
- rollout: bfloat16 [2048, 6144], P('dp', 'tensor'), may hold values from -100 to 100
- lengths: int32 [8, 32], replicated, may hold values from 1 to 8, as said below
- packing: int32 [256], replicated, may hold values from 0 to 255, as said below
- norm_gain: float32 [6144], replicated, may hold values from 0.5 to 4
- query_weight: bfloat16 [6144, 1024], P(None, 'tensor'), may hold values from -0.078125 to 0.078125
- keyval_weight: bfloat16 [6144, 256], P(None, 'tensor'), may hold values from -0.078125 to 0.078125
- out_weight: bfloat16 [1024, 6144], P('tensor'), may hold values from -0.1875 to 0.1875
Outputs:
- layer_out: bfloat16 [2048, 6144], P('dp', 'tensor')
The draws below stay inside these ranges and needn't reach their ends.
Inputs may be any that keep to these rules, and one draw needn't show every extreme that they name: lengths[s, k] is the number of tokens of response k of source s; some response has 8 tokens in every draw. `packing`: a permutation of 0 .. 255; response r comes from source r // 32; every owner receives exactly 32 responses, exactly 4 of them from each source.
All inputs are finite; a program needn't handle non-finite values.
Results may differ from the reference program's by a relative error of at most 0.015.
Values may be sent and summed in bfloat16 or wider, within the bound.
A program may use at most 64 MiB of HBM per device.

```python
import math
import jax
import jax.numpy as jnp
from jax import lax

D = 6144
HD = 128
HQ_DEV = 2
GROUP = 8
MAXLEN = 8
RPS = 32
HEADS = 8
KV_HEADS = 1
L = 256
N_DP = 8
N_TENSOR = 4


def draw_lengths(key, part):
    drawn = jax.random.randint(jax.random.fold_in(key, 11), (N_DP * RPS,), 1, MAXLEN + 1)
    longest = jax.random.randint(jax.random.fold_in(key, 12), (), 0, N_DP * RPS)
    flattened = jnp.where(jnp.arange(N_DP * RPS) == longest, MAXLEN, drawn)
    return flattened.reshape(N_DP, RPS).astype(jnp.int32)


def draw_packing(key, part):
    response_count = N_DP * RPS
    owner_order = jax.random.permutation(jax.random.fold_in(key, 21), N_DP)
    source = jnp.arange(response_count) // RPS
    within = jnp.arange(response_count) % RPS
    target = owner_order[(source + within) % N_DP]
    tiebreak = jax.random.permutation(jax.random.fold_in(key, 22), response_count)
    sort_key = target * response_count + tiebreak
    return jnp.argsort(sort_key).astype(jnp.int32)


def draw_rollout(key, part):
    noise = jax.random.normal(jax.random.fold_in(key, 31), (N_DP * L, D), jnp.float32)
    return jnp.clip(noise, -100.0, 100.0).astype(jnp.bfloat16)


def draw_norm_gain(key, part):
    drawn = 1.0 + 0.1 * jax.random.normal(jax.random.fold_in(key, 42), (D,), jnp.float32)
    return jnp.clip(drawn, 0.5, 4.0).astype(jnp.float32)


def shard_levels(rng, shape, cuts, least, high):
    gain, own = 1.0, jax.random.fold_in(rng, 6)
    for axis_at, blocks in cuts:
        steps = jnp.exp(jax.random.uniform(jax.random.fold_in(own, axis_at), (blocks,), jnp.float32, least / len(cuts), high / len(cuts)))
        gain = gain * jnp.repeat(steps, shape[axis_at] // blocks).reshape([-1 if axis == axis_at else 1 for axis in range(len(shape))])
    return gain


def centred(own_key, shape, scale, most, shards=(), kind=jnp.bfloat16):
    gain = shard_levels(own_key, shape, shards, -0.22, 0.18) if shards else 1.0
    array = jax.random.normal(own_key, shape, jnp.float32) * scale * gain
    return jnp.minimum(jnp.maximum(array, -most), most).astype(kind)


def setup_inputs(seed: int = 0) -> dict:
    key_of = jax.random.split(jax.random.key(seed), 8)
    rollout = draw_rollout(jax.random.fold_in(key_of[7], 71), 0)
    lengths = draw_lengths(jax.random.fold_in(key_of[7], 71), 0)
    packing = draw_packing(jax.random.fold_in(key_of[7], 71), 0)
    norm_gain = draw_norm_gain(jax.random.fold_in(key_of[7], 71), 0)
    query_weight = centred(key_of[4], (D, HEADS * HD), D ** -0.5, 0.078125, ((1, 4),))
    keyval_weight = centred(key_of[5], (D, 2 * KV_HEADS * HD), D ** -0.5, 0.078125, ((1, 4),))
    out_weight = centred(key_of[6], (HEADS * HD, D), (HEADS * HD) ** -0.5, 0.1875, ((0, 4),))
    return {"rollout": rollout, "lengths": lengths, "packing": packing, "norm_gain": norm_gain, "query_weight": query_weight, "keyval_weight": keyval_weight, "out_weight": out_weight}


epsilon = 1e-05
rope_base = 500000.0

def owner_map(lengths, packing, owner_id, pack_len):
    per_source = lengths.shape[1]
    chosen = lax.dynamic_slice_in_dim(packing, owner_id * per_source, per_source)
    ordered = jnp.take(lengths.reshape(-1), chosen)
    doc_start = jnp.cumsum(ordered) - ordered
    places = jnp.arange(pack_len, dtype=jnp.int32)
    inside = (places[:, None] >= doc_start[None, :]) & (places[:, None] < (doc_start + ordered)[None, :])
    is_valid = jnp.any(inside, axis=1)
    slot_of = lax.optimization_barrier(jnp.sum(jnp.where(inside, jnp.arange(per_source, dtype=jnp.int32)[None, :], 0), axis=1)).astype(jnp.int32)
    response = jnp.take(chosen, slot_of)
    position = jnp.where(is_valid, places - jnp.take(doc_start, slot_of), 0).astype(jnp.int32)
    doc_id = jnp.where(is_valid, slot_of, per_source).astype(jnp.int32)
    return (response, position, doc_id, is_valid)

def rotate(values, position, head_dim):
    half_dim = head_dim // 2
    frequency = rope_base ** (-jnp.arange(half_dim, dtype=jnp.float32) * 2.0 / head_dim)
    angles = position.astype(jnp.float32)[:, None] * frequency[None, :]
    cosine = jnp.concatenate([jnp.cos(angles), jnp.cos(angles)], axis=1)[:, None, :]
    sine_table = jnp.concatenate([jnp.sin(angles), jnp.sin(angles)], axis=1)[:, None, :]
    turned = jnp.concatenate([-values[..., half_dim:], values[..., :half_dim]], axis=-1)
    return values * cosine + turned * sine_table

def reference(rollout, lengths, packing, norm_gain, query_weight, keyval_weight, out_weight):
    per_source = lengths.shape[1]
    source_start = (jnp.cumsum(lengths, axis=1) - lengths).reshape(-1).astype(jnp.int32)
    kv_count = keyval_weight.shape[1] // (2 * HD)
    head_count = query_weight.shape[1] // HD

    def one_owner(owner_id):
        response, position, doc_id, is_valid = owner_map(lengths, packing, owner_id, L)
        global_row = response // per_source * L + jnp.take(source_start, response) + position
        packed = jnp.where(is_valid[:, None], jnp.take(rollout, global_row.astype(jnp.int32), axis=0), jnp.zeros((), jnp.bfloat16))
        widened = packed.astype(jnp.float32)
        inverse = lax.rsqrt(lax.optimization_barrier(jnp.mean(widened * widened, axis=1)) + epsilon)
        scaled = (widened * norm_gain[None, :]).astype(jnp.bfloat16)
        queries = jnp.dot(scaled, query_weight, preferred_element_type=jnp.float32) * inverse[:, None]
        keyval = (jnp.dot(scaled, keyval_weight, preferred_element_type=jnp.float32) * inverse[:, None]).astype(jnp.bfloat16)
        q_rot = rotate(queries.reshape(L, head_count, HD), position, HD).astype(jnp.bfloat16)
        k_rot = rotate(keyval[:, :kv_count * HD].astype(jnp.float32).reshape(L, kv_count, HD), position, HD).astype(jnp.bfloat16)
        value_heads = keyval[:, kv_count * HD:].reshape(L, kv_count, HD)
        shared_head = jnp.arange(head_count, dtype=jnp.int32) // GROUP
        key_full = k_rot[:, shared_head]
        value_full = value_heads[:, shared_head]
        scores = jnp.einsum('qhd,khd->hqk', q_rot.astype(jnp.float32), key_full.astype(jnp.float32)) / math.sqrt(HD)
        places = jnp.arange(L, dtype=jnp.int32)
        allowed = (doc_id[:, None] == doc_id[None, :]) & (places[None, :] <= places[:, None])
        masked = jnp.where(allowed[None], scores, -jnp.inf)
        row_max = lax.optimization_barrier(jnp.max(masked, axis=2, keepdims=True))
        exponent = jnp.exp(masked - row_max)
        weights = (exponent / lax.optimization_barrier(jnp.sum(exponent, axis=2, keepdims=True))).astype(jnp.bfloat16)
        context = jnp.einsum('hqk,khd->qhd', weights.astype(jnp.float32), value_full.astype(jnp.float32))
        context = context.astype(jnp.bfloat16).reshape(L, head_count * HD)
        groups = context.reshape(L, N_TENSOR, HQ_DEV * HD).transpose(1, 0, 2)
        out_groups = out_weight.reshape(N_TENSOR, HQ_DEV * HD, D)

        def add_group(summed, operands):
            portion = jnp.dot(operands[0], operands[1], preferred_element_type=jnp.float32).astype(jnp.bfloat16)
            portion = lax.optimization_barrier(portion)
            return (summed + portion.astype(jnp.float32), None)
        summed, unused = lax.scan(add_group, jnp.zeros((L, D), jnp.float32), (groups, out_groups))
        return jnp.where(is_valid[:, None], summed + widened, 0.0).astype(jnp.bfloat16)
    outputs = lax.map(one_owner, jnp.arange(N_DP, dtype=jnp.int32))
    return outputs.reshape(N_DP * L, D)
```

```python
import functools
import math

import numpy as np
import jax
import jax.numpy as jnp
from jax import lax
from jax.experimental import pallas as pl
from jax.experimental.pallas import tpu as pltpu
from jax.sharding import PartitionSpec as P

D = 6144
HD = 128
HQ_DEV = 2
GROUP = 8


epsilon = 1e-05
rope_base = 500000.0


def owner_map(lengths, packing, owner_id, pack_len):
    per_source = lengths.shape[1]
    chosen = lax.dynamic_slice_in_dim(packing, owner_id * per_source, per_source)
    ordered = jnp.take(lengths.reshape(-1), chosen)
    doc_start = jnp.cumsum(ordered) - ordered
    places = jnp.arange(pack_len, dtype=jnp.int32)
    inside = (places[:, None] >= doc_start[None, :]) & (
        places[:, None] < (doc_start + ordered)[None, :]
    )
    is_valid = jnp.any(inside, axis=1)
    slot_of = jnp.sum(
        jnp.where(inside, jnp.arange(per_source, dtype=jnp.int32)[None, :], 0), axis=1
    )
    response = jnp.take(chosen, slot_of)
    position = jnp.where(is_valid, places - jnp.take(doc_start, slot_of), 0)
    doc_id = jnp.where(is_valid, slot_of, per_source)
    return (response, position, doc_id, is_valid)


def rotate(values, position, head_dim):
    half_dim = head_dim // 2
    frequency = rope_base ** (-jnp.arange(half_dim, dtype=jnp.float32) * 2.0 / head_dim)
    angles = position.astype(jnp.float32)[:, None] * frequency[None, :]
    cosine = jnp.concatenate([jnp.cos(angles), jnp.cos(angles)], axis=1)[:, None, :]
    sine_table = jnp.concatenate([jnp.sin(angles), jnp.sin(angles)], axis=1)[:, None, :]
    turned = jnp.concatenate([-values[..., half_dim:], values[..., :half_dim]], axis=-1)
    return values * cosine + turned * sine_table


def plain_body(rollout, lengths, packing, norm_gain, query_weight, keyval_weight, out_weight):
    owner_id = lax.axis_index("dp")
    tensor_index = lax.axis_index("tensor")
    tensor_count = lax.axis_size("tensor")
    pack_len = rollout.shape[0]
    per_source = lengths.shape[1]
    response, position, doc_id, is_valid = owner_map(lengths, packing, owner_id, pack_len)
    source_start = jnp.cumsum(lengths, axis=1) - lengths
    global_row = (
        response // per_source * pack_len + jnp.take(source_start.reshape(-1), response) + position
    )
    portion = lax.all_gather(rollout, "dp", axis=0, tiled=True)
    within = is_valid & (global_row >= 0) & (global_row < portion.shape[0])
    picked = jnp.take(portion, jnp.clip(global_row, 0, portion.shape[0] - 1), axis=0)
    packed = jnp.where(within[:, None], picked, jnp.zeros_like(rollout))
    widened = lax.all_gather(packed, "tensor", axis=1, tiled=True).astype(jnp.float32)
    scaled = (widened * norm_gain[None, :]).astype(jnp.bfloat16)
    query_acc = jnp.dot(scaled, query_weight, preferred_element_type=jnp.float32)
    keyval_acc = jnp.dot(scaled, keyval_weight, preferred_element_type=jnp.float32)
    squares = jnp.sum(widened * widened, axis=1)
    query_acc, keyval_acc, squares = (query_acc, keyval_acc, squares)
    inverse = lax.rsqrt(squares / D + epsilon)
    queries = query_acc * inverse[:, None]
    keyval_share = (keyval_acc * inverse[:, None]).astype(jnp.bfloat16)
    keyval_all = lax.all_gather(keyval_share, "tensor", axis=1, tiled=True)
    kv_count = keyval_weight.shape[1] * tensor_count // (2 * HD)
    shared_head = tensor_index * HQ_DEV // GROUP
    keys = lax.dynamic_slice_in_dim(keyval_all, shared_head * HD, HD, 1)
    values = lax.dynamic_slice_in_dim(keyval_all, (kv_count + shared_head) * HD, HD, 1)
    q_rot = rotate(queries.reshape(pack_len, HQ_DEV, HD), position, HD).astype(jnp.bfloat16)
    k_rot = rotate(keys.astype(jnp.float32)[:, None, :], position, HD)[:, 0, :].astype(jnp.bfloat16)
    scores = jnp.einsum(
        "qhd,kd->hqk", q_rot, k_rot, preferred_element_type=jnp.float32
    ) / math.sqrt(HD)
    places = jnp.arange(pack_len, dtype=jnp.int32)
    allowed = (doc_id[:, None] == doc_id[None, :]) & (places[None, :] <= places[:, None])
    masked = jnp.where(allowed[None], scores, -jnp.inf)
    row_max = jnp.max(masked, axis=2, keepdims=True)
    exponent = jnp.exp(masked - row_max)
    weights = (exponent / jnp.sum(exponent, axis=2, keepdims=True)).astype(jnp.bfloat16)
    context = jnp.einsum("hqk,kd->qhd", weights, values, preferred_element_type=jnp.float32)
    context = context.astype(jnp.bfloat16).reshape(pack_len, HQ_DEV * HD)
    partial_sum = jnp.dot(context, out_weight, preferred_element_type=jnp.float32)
    summed = lax.psum_scatter(
        partial_sum.astype(jnp.bfloat16), "tensor", scatter_dimension=1, tiled=True
    ).astype(jnp.float32)
    result = jnp.where(is_valid[:, None], summed + packed.astype(jnp.float32), 0.0)
    return result.astype(jnp.bfloat16)


MESH = pl.DeviceIdType.MESH
CORES = 2
SIDE = 2


def aligned(index, size):
    return pl.multiple_of(index * size, size)


def fused_kernel(
    cfg, pk_hbm, len_hbm, gain_hbm, tab_hbm, roll_hbm, w_in, k_in, o_in, out,
    pk_buf, len_buf, gain, tab, wbuf, kbuf, obuf, roll_in, sendb, recvb, packed, scaled, q_rot, kv_part, kv_recv, kv_all, ctx,
    pos_buf, valid_buf, cos_buf, sin_buf, inv_buf, mask_buf, fold_buf, sq_part, sq_recv, score_part, score_recv,
    send_sems, recv_sems, local_sems,
):
    n_dp, n_t, length, feat, per_source = cfg
    chips = n_dp // CORES
    w_sub = feat // n_dp
    kd = k_in.shape[0]
    k_rows, k_cols = kd // chips, feat // CORES
    o_rows = o_in.shape[0]
    o_sub = o_rows // n_dp
    block = length // n_dp
    most = length // per_source
    rows = length // n_t
    qd = w_in.shape[1]
    heads = n_t * qd // HD
    half = length // 2
    me = lax.axis_index("dp")
    t = lax.axis_index("tensor")
    core = lax.rem(me, CORES)
    chip = lax.div(me, CORES)
    partner = chip * CORES + (CORES - 1 - core)
    near_x = chip + 1 - 2 * lax.rem(chip, SIDE)
    near_y = chip + SIDE - 2 * SIDE * lax.div(chip, SIDE)
    first_chip = near_x + core * (near_y - near_x)
    other_chip = near_y + core * (near_x - near_y)
    far_chip = chips - 1 - chip

    def t_at(k):
        return lax.rem(t + k, n_t)

    barrier = pltpu.get_barrier_semaphore()
    for k in range(1, n_dp):
        pl.semaphore_signal(
            barrier, inc=1, device_id=(lax.rem(me + k, n_dp), t), device_id_type=MESH
        )
    for k in range(1, n_t):
        pl.semaphore_signal(barrier, inc=1, device_id=(me, t_at(k)), device_id_type=MESH)

    small = [
        pltpu.make_async_copy(source, target, local_sems.at[4 + i])
        for i, (source, target) in enumerate(
            (
                (pk_hbm, pk_buf),
                (len_hbm, len_buf),
                (gain_hbm.at[:, pl.ds(aligned(t, feat), feat)], gain),
                (tab_hbm, tab),
            )
        )
    ]
    load = pltpu.make_async_copy(roll_hbm, roll_in, local_sems.at[2])
    own_w = pltpu.make_async_copy(
        w_in.at[pl.ds(aligned(t, feat), feat)], wbuf.at[t], local_sems.at[0]
    )
    own_k = pltpu.make_async_copy(
        k_in.at[:, pl.ds(aligned(t, feat), feat)],
        kbuf.at[pl.ds(aligned(t, kd), kd)],
        local_sems.at[3],
    )
    own_o = pltpu.make_async_copy(
        o_in.at[:, pl.ds(aligned(t, feat), feat)], obuf.at[t], local_sems.at[1]
    )
    for copy in [*small, load, own_k, own_w, own_o]:
        copy.start()

    started = []

    def send(source, target, device):
        at = len(started)
        copy = pltpu.make_async_remote_copy(
            src_ref=source,
            dst_ref=target,
            send_sem=send_sems.at[at],
            recv_sem=recv_sems.at[at],
            device_id=device,
            device_id_type=MESH,
        )
        copy.start()
        started.append(copy)
        return copy

    def w_at(u, h, c):
        return wbuf.at[u, pl.ds(aligned(h * CORES + c, w_sub), w_sub)]

    def k_at(u, h, c):
        return kbuf.at[
            pl.ds(aligned(u * chips + h, k_rows), k_rows), pl.ds(aligned(c, k_cols), k_cols)
        ]

    def o_at(u, h, c):
        return obuf.at[u, pl.ds(aligned(h * CORES + c, o_sub), o_sub)]

    down = lax.broadcasted_iota(jnp.int32, (length, length), 0).astype(jnp.float32)
    across = lax.broadcasted_iota(jnp.int32, (length, length), 1).astype(jnp.float32)

    def part(value, size):
        return jnp.floor((value + 0.5) * (1.0 / size))

    def pick(mask, value, axis):
        return jnp.sum(jnp.where(mask, value, 0.0), axis=axis, keepdims=True)

    same = part(down, per_source) == part(across, per_source)
    diagonal = down == across
    for copy in small:
        copy.wait()
    len_all = len_buf[...].astype(jnp.float32)
    source_of = part(down[:, :1], per_source)
    table = jnp.zeros((length, per_source), jnp.float32)
    for i in range(n_dp):
        table = jnp.where(source_of == float(i), len_all[i : i + 1, :], table)
    within = down[:, :per_source] - source_of * per_source
    len_c = pick(across[:, :per_source] == within, table, 1)
    len_r = pick(diagonal, len_c, 0)
    pk_r = pk_buf[...].astype(jnp.float32)
    pk_c = pick(diagonal, pk_r, 1)
    src_start = pick(same & (across < down), len_r, 1)
    chosen = down == pk_r
    q_len_r = pick(chosen, len_c, 0)
    q_start_r = pick(chosen, src_start, 0)
    q_len_c = pick(across == pk_c, len_r, 1)
    earlier = same & (down < across)
    doc_start_r = pick(earlier, q_len_c, 0)
    q_src_r = part(pk_r, per_source)
    slot_r = pick(earlier & (part(pk_c, per_source) == q_src_r), 1.0, 0)
    mine = me.astype(jnp.float32)
    across_1 = across[:1]
    down_1 = down[:, :1]
    owner_r = part(across_1, per_source)
    target = jnp.where(q_src_r == mine, owner_r * (per_source // n_dp) + slot_r, -1.0)
    group = part(down_1, most)
    match = target == group
    token = down_1 - group * most
    row_sent = jnp.where(token < pick(match, q_len_r, 1), pick(match, q_start_r, 1) + token, -1.0)
    take_send = (across == row_sent).astype(jnp.float32).astype(jnp.bfloat16)

    tile = 256
    tiles = feat // tile

    def send_tile(i, carry):
        at = pl.ds(aligned(i, tile), tile)
        sendb[:, at] = jnp.dot(
            take_send, roll_in[:, at], preferred_element_type=jnp.float32
        ).astype(jnp.bfloat16)
        return carry

    load.wait()
    lax.fori_loop(0, tiles, send_tile, 0)

    pl.semaphore_wait(barrier, n_dp + n_t - 2)

    others = range(1, n_t)
    w_first, k_first, o_first = {}, {}, {}
    for k in others:
        to = t_at(k)
        k_first[k] = send(
            k_in.at[
                pl.ds(aligned(chip, k_rows), k_rows),
                pl.ds(aligned(to * CORES + core, k_cols), k_cols),
            ],
            k_at(t, chip, core),
            (me, to),
        )
    rows_of = []
    for k in range(1, n_dp):
        to = lax.rem(me + k, n_dp)
        rows_of.append(
            send(
                sendb.at[pl.ds(aligned(to, block), block)],
                recvb.at[pl.ds(aligned(me, block), block)],
                (to, t),
            )
        )
    for k in others:
        to = t_at(k)
        w_first[k] = send(
            w_in.at[pl.ds(aligned(to * n_dp + me, w_sub), w_sub)], w_at(t, chip, core), (me, to)
        )

    def send_o(k):
        to = t_at(k)
        o_first[k] = send(
            o_in.at[pl.ds(aligned(me, o_sub), o_sub), pl.ds(aligned(to, feat), feat)],
            o_at(t, chip, core),
            (me, to),
        )

    send_o(1)

    keep = pl.ds(aligned(me, block), block)
    recvb[keep, :] = sendb[keep, :]
    inside = (owner_r == mine) & (doc_start_r <= down) & (down < doc_start_r + q_len_r)
    is_valid = pick(inside, 1.0, 1)
    position = (down_1 - pick(inside, doc_start_r, 1)) * is_valid
    row_got = jnp.where(
        is_valid > 0.0, pick(inside, q_src_r * block + slot_r * most, 1) + position, -1.0
    )
    take_recv = (across == row_got).astype(jnp.float32).astype(jnp.bfloat16)
    pos = jnp.broadcast_to(position, (length, HD))
    pos_buf[...] = pos
    valid_buf[...] = jnp.broadcast_to(is_valid, (length, HD))
    cosine = jnp.zeros((length, HD), jnp.float32)
    sine = jnp.zeros((length, HD), jnp.float32)
    for m in range(most):
        at_m = pos == float(m)
        cosine = jnp.where(at_m, tab[m : m + 1, :], cosine)
        sine = jnp.where(at_m, tab[most + m : most + m + 1, :], sine)
    cos_buf[...] = cosine
    sin_buf[...] = sine
    mask_buf[...] = ((across <= down) & (across >= down - position)).astype(jnp.float32)
    fold_down = lax.broadcasted_iota(jnp.int32, (length, HD), 0)
    fold_across = lax.broadcasted_iota(jnp.int32, (length, HD), 1)
    fold_buf[...] = (
        (lax.rem(fold_down, most) == lax.rem(fold_across, most))
        .astype(jnp.float32)
        .astype(jnp.bfloat16)
    )

    def spread(at, first, j):
        first[j].wait_recv()
        ref = at(t_at(n_t - j), chip, core)
        return [
            send(ref, ref, (first_chip * CORES + core, t)),
            send(ref, ref, (other_chip * CORES + core, t)),
            send(ref, ref, (partner, t)),
        ]

    def relay(at, hops, j):
        hops[0].wait_recv()
        ref = at(t_at(n_t - j), first_chip, core)
        hops.append(send(ref, ref, (other_chip * CORES + core, t)))
        hops.append(send(ref, ref, (partner, t)))

    def settle(at, hops, j):
        for near, source in ((1, other_chip), (3, far_chip)):
            hops[near].wait_recv()
            ref = at(t_at(n_t - j), source, core)
            hops.append(send(ref, ref, (partner, t)))

    def finish(hops):
        for at in (2, 4, 5, 6):
            hops[at].wait_recv()

    k_hops = {j: spread(k_at, k_first, j) for j in others}
    for j in others:
        relay(k_at, k_hops[j], j)
    w_hops = {1: spread(w_at, w_first, 1)}

    for copy in rows_of:
        copy.wait_recv()

    def pack_tile(i, total):
        at = pl.ds(aligned(i, tile), tile)
        x = jnp.dot(take_recv, recvb[:, at], preferred_element_type=jnp.float32)
        packed[:, at] = x.astype(jnp.bfloat16)
        g = gain[:, at]
        scaled[:, at] = (x * g).astype(jnp.bfloat16)
        return total + jnp.sum(x * x, axis=1, keepdims=True)

    squares = lax.fori_loop(0, tiles, pack_tile, jnp.zeros((length, 1), jnp.float32))
    sq_part[...] = jnp.broadcast_to(pick(diagonal, squares, 0), (8, length))
    sq_sent = [send(sq_part, sq_recv.at[k - 1], (me, t_at(k))) for k in others]

    for j in others:
        settle(k_at, k_hops[j], j)
    own_k.wait()
    for j in others:
        finish(k_hops[j])
    kv_sent = []
    for c in range(2):
        cols = slice(c * HD, (c + 1) * HD)
        kv_part[:, cols] = lax.dot_general(
            scaled[...], kbuf[cols, :], (((1,), (1,)), ((), ())),
            preferred_element_type=jnp.float32,
        ).astype(jnp.bfloat16)
        for k in others:
            to = t_at(k)
            kv_sent.append(
                send(
                    kv_part.at[pl.ds(aligned(to, rows), rows), cols],
                    kv_recv.at[k - 1, :, cols],
                    (me, to),
                )
            )
    send_o(2)
    relay(w_at, w_hops[1], 1)
    w_hops[2] = spread(w_at, w_first, 2)
    relay(w_at, w_hops[2], 2)

    for copy in sq_sent:
        copy.wait_recv()
    sq = sq_part[:1, :]
    for k in range(n_t - 1):
        sq += sq_recv[k, :1, :]
    inverse = lax.rsqrt(sq / (feat * n_t) + epsilon)
    inv_buf[...] = jnp.broadcast_to(pick(diagonal, inverse, 1), (length, HD))

    def turn(v, c, s):
        return v * c + pltpu.roll(v, HD // 2, 1) * s

    def project(u):
        q = jnp.dot(scaled[...], wbuf[u], preferred_element_type=jnp.float32)
        for h in range(qd // HD):
            part_q = q[:, h * HD : (h + 1) * HD] * inv_buf[...]
            q_rot[:, pl.ds(aligned(u * (qd // HD) + h, HD), HD)] = turn(
                part_q, cos_buf[...], sin_buf[...]
            ).astype(jnp.bfloat16)

    own_w.wait()
    project(t)

    mine_rows = pl.ds(aligned(t, rows), rows)
    gathers = []
    for c in range(2):
        cols = slice(c * HD, (c + 1) * HD)
        for copy in kv_sent[c * (n_t - 1) : (c + 1) * (n_t - 1)]:
            copy.wait_recv()
        kv = kv_part[mine_rows, cols].astype(jnp.float32)
        for k in range(n_t - 1):
            kv += kv_recv[k, :, cols].astype(jnp.float32)
        kv = (kv * inv_buf[mine_rows, :]).astype(jnp.bfloat16)
        if c == 0:
            kv = turn(
                kv.astype(jnp.float32), cos_buf[mine_rows, :], sin_buf[mine_rows, :]
            ).astype(jnp.bfloat16)
        kv_all[mine_rows, cols] = kv
        at = kv_all.at[mine_rows, cols]
        gathers.append([send(at, at, (me, t_at(k))) for k in others])
    send_o(3)

    w_hops[3] = spread(w_at, w_first, 3)
    relay(w_at, w_hops[3], 3)
    o_hops = {1: spread(o_at, o_first, 1)}
    for j in others:
        settle(w_at, w_hops[j], j)
        finish(w_hops[j])
        project(t_at(n_t - j))
        if j == 1:
            o_hops[2] = spread(o_at, o_first, 2)
        if j == 2:
            relay(o_at, o_hops[1], 1)

    for copy in gathers[0]:
        copy.wait_recv()
    lane = lax.broadcasted_iota(jnp.int32, (half, HD), 1)
    line = lax.broadcasted_iota(jnp.int32, (half, HD), 0)
    cell = lax.div(lane, most)
    compact = jnp.zeros((half, HD), jnp.float32)
    for h in range(heads):
        scores = lax.dot_general(
            q_rot[:, h * HD : (h + 1) * HD], kv_all[:, :HD], (((1,), (1,)), ((), ())),
            preferred_element_type=jnp.float32,
        )
        scores = (scores * mask_buf[...]).astype(jnp.bfloat16)
        folded = jnp.dot(scores, fold_buf[...], preferred_element_type=jnp.float32)
        compact = jnp.where(cell == h, folded[:half], compact)
        compact = jnp.where(cell == heads + h, folded[half:], compact)
    score_part[...] = compact.astype(jnp.bfloat16)
    score_sent = [send(score_part, score_recv.at[k - 1], (me, t_at(k))) for k in others]

    o_hops[3] = spread(o_at, o_first, 3)
    relay(o_at, o_hops[2], 2)
    relay(o_at, o_hops[3], 3)
    for j in others:
        settle(o_at, o_hops[j], j)

    for copy in score_sent:
        copy.wait_recv()
    total = score_part[...].astype(jnp.float32)
    for k in range(n_t - 1):
        total += score_recv[k].astype(jnp.float32)
    place = jnp.where(cell < heads, pos_buf[:half, :], pos_buf[half:, :])
    back = lax.rem(line - lane + HD, most).astype(jnp.float32)
    total = jnp.where(back <= place, total * (1.0 / math.sqrt(HD)), -jnp.inf)

    def around(value, combine):
        step = 1
        while step < most:
            low = lax.rem(lax.div(lane, step), 2) == 0
            value = combine(
                value,
                jnp.where(low, pltpu.roll(value, HD - step, 1), pltpu.roll(value, step, 1)),
            )
            step *= 2
        return value

    exponent = jnp.exp(total - around(total, jnp.maximum))
    weights = exponent / around(exponent, jnp.add)
    for copy in gathers[1]:
        copy.wait_recv()
    for h in range(heads):
        chosen_w = jnp.concatenate(
            [jnp.where(cell == h, weights, 0.0), jnp.where(cell == heads + h, weights, 0.0)], axis=0
        ).astype(jnp.bfloat16)
        dense = lax.dot_general(
            chosen_w, fold_buf[...], (((1,), (1,)), ((), ())), preferred_element_type=jnp.float32
        )
        dense = (dense * mask_buf[...]).astype(jnp.bfloat16)
        ctx[:, h * HD : (h + 1) * HD] = jnp.dot(
            dense, kv_all[:, HD:], preferred_element_type=jnp.float32
        ).astype(jnp.bfloat16)

    own_o.wait()
    for j in others:
        finish(o_hops[j])

    def out_tile(i, carry):
        at = pl.ds(aligned(i, tile), tile)
        result = packed[:, at].astype(jnp.float32)
        for u in range(n_t):
            result += jnp.dot(
                ctx[:, u * o_rows : (u + 1) * o_rows],
                obuf[u, :, at],
                preferred_element_type=jnp.float32,
            )
        out[:, at] = jnp.where(valid_buf[:, :1] > 0.0, result, 0.0).astype(jnp.bfloat16)
        return carry

    lax.fori_loop(0, tiles, out_tile, 0)
    for copy in started:
        copy.wait_send()


def fused_body(rollout, lengths, packing, norm_gain, query_weight, keyval_weight, out_weight):
    n_dp, n_t = lax.axis_size("dp"), lax.axis_size("tensor")
    length, feat = rollout.shape
    per_source = lengths.shape[1]
    most = length // per_source
    qd, kd = query_weight.shape[1], keyval_weight.shape[1]
    frequency = np.float32(rope_base) ** (-np.arange(HD // 2, dtype=np.float32) * 2.0 / HD)
    angles = np.arange(most, dtype=np.float32)[:, None] * frequency[None, :].astype(np.float32)
    cos_tab = np.concatenate([np.cos(angles)] * 2, axis=1).astype(np.float32)
    sin_tab = np.concatenate([-np.sin(angles), np.sin(angles)], axis=1).astype(np.float32)
    rows = length // n_t
    chips = n_dp // CORES
    copies = 3 * (n_t - 1) * (1 + chips - 1 + chips) + (n_dp - 1) + 6 * (n_t - 1)
    vmem = pl.BlockSpec(memory_space=pltpu.VMEM)
    hbm = pl.BlockSpec(memory_space=pl.ANY)
    bf, f32 = jnp.bfloat16, jnp.float32
    return pl.pallas_call(
        functools.partial(fused_kernel, (n_dp, n_t, length, feat, per_source)),
        out_shape=jax.ShapeDtypeStruct((length, feat), bf),
        in_specs=[hbm] * 8,
        out_specs=vmem,
        scratch_shapes=[
            pltpu.VMEM((1, packing.shape[0]), jnp.int32),
            pltpu.VMEM(lengths.shape, jnp.int32),
            pltpu.VMEM((1, feat), f32),
            pltpu.VMEM((2 * most, HD), f32),
            pltpu.VMEM((n_t, feat, qd), bf),
            pltpu.VMEM((n_t * kd, feat), bf),
            pltpu.VMEM((n_t, out_weight.shape[0], feat), bf),
            pltpu.VMEM((length, feat), bf),
            pltpu.VMEM((length, feat), bf),
            pltpu.VMEM((length, feat), bf),
            pltpu.VMEM((length, feat), bf),
            pltpu.VMEM((length, feat), bf),
            pltpu.VMEM((length, n_t * qd), bf),
            pltpu.VMEM((length, 2 * HD), bf),
            pltpu.VMEM((n_t - 1, rows, 2 * HD), bf),
            pltpu.VMEM((length, 2 * HD), bf),
            pltpu.VMEM((length, n_t * qd), bf),
            pltpu.VMEM((length, HD), f32),
            pltpu.VMEM((length, HD), f32),
            pltpu.VMEM((length, HD), f32),
            pltpu.VMEM((length, HD), f32),
            pltpu.VMEM((length, HD), f32),
            pltpu.VMEM((length, length), f32),
            pltpu.VMEM((length, HD), bf),
            pltpu.VMEM((8, length), f32),
            pltpu.VMEM((n_t - 1, 8, length), f32),
            pltpu.VMEM((length // 2, HD), bf),
            pltpu.VMEM((n_t - 1, length // 2, HD), bf),
            pltpu.SemaphoreType.DMA((copies,)),
            pltpu.SemaphoreType.DMA((copies,)),
            pltpu.SemaphoreType.DMA((8,)),
        ],
        compiler_params=pltpu.CompilerParams(
            collective_id=0, has_side_effects=True, vmem_limit_bytes=60 * 1024 * 1024
        ),
    )(
        packing[None, :], lengths, norm_gain[None, :],
        jnp.asarray(np.concatenate([cos_tab, sin_tab])), rollout, query_weight,
        keyval_weight.T, out_weight,
    )


def body(rollout, lengths, packing, norm_gain, query_weight, keyval_weight, out_weight):
    n_dp, n_t = lax.axis_size("dp"), lax.axis_size("tensor")
    length, feat = rollout.shape
    per_source = lengths.shape[1]
    qd, kd = query_weight.shape[1], keyval_weight.shape[1]
    fits = (
        kd * n_t == 2 * HD
        and n_t == 4
        and n_dp == SIDE * SIDE * CORES
        and qd % HD == 0
        and n_t * qd // HD <= GROUP
        and per_source * 8 == length
        and n_t * qd // HD * 8 * 2 == HD
        and kd % (16 * n_dp // CORES) == 0
        and feat % (128 * CORES) == 0
        and length % (n_t * 16) == 0
        and length == 2 * HD
        and packing.shape[0] == length
        and (length // n_dp) % 16 == 0
        and feat % 512 == 0
        and per_source % n_dp == 0
    )
    chosen = fused_body if fits else plain_body
    return chosen(rollout, lengths, packing, norm_gain, query_weight, keyval_weight, out_weight)


def solution(mesh):
    in_specs = (
        P("dp", "tensor"),
        P(),
        P(),
        P(),
        P(None, "tensor"),
        P(None, "tensor"),
        P("tensor", None),
    )
    out_specs = P("dp", "tensor")
    return jax.shard_map(body, mesh=mesh, in_specs=in_specs, out_specs=out_specs, check_vma=False)
```

```python
import functools
import math

import numpy as np
import jax
import jax.numpy as jnp
from jax import lax
from jax.experimental import pallas as pl
from jax.experimental.pallas import tpu as pltpu
from jax.sharding import PartitionSpec as P

D = 6144
HD = 128
HQ_DEV = 2
GROUP = 8


epsilon = 1e-05
rope_base = 500000.0


def owner_map(lengths, packing, owner_id, pack_len):
    per_source = lengths.shape[1]
    chosen = lax.dynamic_slice_in_dim(packing, owner_id * per_source, per_source)
    ordered = jnp.take(lengths.reshape(-1), chosen)
    doc_start = jnp.cumsum(ordered) - ordered
    places = jnp.arange(pack_len, dtype=jnp.int32)
    inside = (places[:, None] >= doc_start[None, :]) & (
        places[:, None] < (doc_start + ordered)[None, :]
    )
    is_valid = jnp.any(inside, axis=1)
    slot_of = jnp.sum(
        jnp.where(inside, jnp.arange(per_source, dtype=jnp.int32)[None, :], 0), axis=1
    )
    response = jnp.take(chosen, slot_of)
    position = jnp.where(is_valid, places - jnp.take(doc_start, slot_of), 0)
    doc_id = jnp.where(is_valid, slot_of, per_source)
    return (response, position, doc_id, is_valid)


def rotate(values, position, head_dim):
    half_dim = head_dim // 2
    frequency = rope_base ** (-jnp.arange(half_dim, dtype=jnp.float32) * 2.0 / head_dim)
    angles = position.astype(jnp.float32)[:, None] * frequency[None, :]
    cosine = jnp.concatenate([jnp.cos(angles), jnp.cos(angles)], axis=1)[:, None, :]
    sine_table = jnp.concatenate([jnp.sin(angles), jnp.sin(angles)], axis=1)[:, None, :]
    turned = jnp.concatenate([-values[..., half_dim:], values[..., :half_dim]], axis=-1)
    return values * cosine + turned * sine_table


def plain_body(rollout, lengths, packing, norm_gain, query_weight, keyval_weight, out_weight):
    owner_id = lax.axis_index("dp")
    tensor_index = lax.axis_index("tensor")
    tensor_count = lax.axis_size("tensor")
    pack_len = rollout.shape[0]
    per_source = lengths.shape[1]
    response, position, doc_id, is_valid = owner_map(lengths, packing, owner_id, pack_len)
    source_start = jnp.cumsum(lengths, axis=1) - lengths
    global_row = (
        response // per_source * pack_len + jnp.take(source_start.reshape(-1), response) + position
    )
    portion = lax.all_gather(rollout, "dp", axis=0, tiled=True)
    within = is_valid & (global_row >= 0) & (global_row < portion.shape[0])
    picked = jnp.take(portion, jnp.clip(global_row, 0, portion.shape[0] - 1), axis=0)
    packed = jnp.where(within[:, None], picked, jnp.zeros_like(rollout))
    widened = lax.all_gather(packed, "tensor", axis=1, tiled=True).astype(jnp.float32)
    scaled = (widened * norm_gain[None, :]).astype(jnp.bfloat16)
    query_acc = jnp.dot(scaled, query_weight, preferred_element_type=jnp.float32)
    keyval_acc = jnp.dot(scaled, keyval_weight, preferred_element_type=jnp.float32)
    squares = jnp.sum(widened * widened, axis=1)
    query_acc, keyval_acc, squares = (query_acc, keyval_acc, squares)
    inverse = lax.rsqrt(squares / D + epsilon)
    queries = query_acc * inverse[:, None]
    keyval_share = (keyval_acc * inverse[:, None]).astype(jnp.bfloat16)
    keyval_all = lax.all_gather(keyval_share, "tensor", axis=1, tiled=True)
    kv_count = keyval_weight.shape[1] * tensor_count // (2 * HD)
    shared_head = tensor_index * HQ_DEV // GROUP
    keys = lax.dynamic_slice_in_dim(keyval_all, shared_head * HD, HD, 1)
    values = lax.dynamic_slice_in_dim(keyval_all, (kv_count + shared_head) * HD, HD, 1)
    q_rot = rotate(queries.reshape(pack_len, HQ_DEV, HD), position, HD).astype(jnp.bfloat16)
    k_rot = rotate(keys.astype(jnp.float32)[:, None, :], position, HD)[:, 0, :].astype(jnp.bfloat16)
    scores = jnp.einsum(
        "qhd,kd->hqk", q_rot, k_rot, preferred_element_type=jnp.float32
    ) / math.sqrt(HD)
    places = jnp.arange(pack_len, dtype=jnp.int32)
    allowed = (doc_id[:, None] == doc_id[None, :]) & (places[None, :] <= places[:, None])
    masked = jnp.where(allowed[None], scores, -jnp.inf)
    row_max = jnp.max(masked, axis=2, keepdims=True)
    exponent = jnp.exp(masked - row_max)
    weights = (exponent / jnp.sum(exponent, axis=2, keepdims=True)).astype(jnp.bfloat16)
    context = jnp.einsum("hqk,kd->qhd", weights, values, preferred_element_type=jnp.float32)
    context = context.astype(jnp.bfloat16).reshape(pack_len, HQ_DEV * HD)
    partial_sum = jnp.dot(context, out_weight, preferred_element_type=jnp.float32)
    summed = lax.psum_scatter(
        partial_sum.astype(jnp.bfloat16), "tensor", scatter_dimension=1, tiled=True
    ).astype(jnp.float32)
    result = jnp.where(is_valid[:, None], summed + packed.astype(jnp.float32), 0.0)
    return result.astype(jnp.bfloat16)


MESH = pl.DeviceIdType.MESH
CORES = 2
SIDE = 2


def aligned(index, size):
    return pl.multiple_of(index * size, size)


def fused_kernel(
    cfg, pk_hbm, len_hbm, gain_hbm, tab_hbm, roll_hbm, w_in, k_in, o_in, out,
    pk_buf, len_buf, gain, tab, wbuf, kbuf, obuf, roll_in, sendb, recvb, packed, scaled, q_rot, kv_part, kv_recv, kv_all, ctx,
    pos_buf, valid_buf, cos_buf, sin_buf, inv_buf, mask_buf, fold_buf, sq_part, sq_recv, score_part, score_recv,
    send_sem, recv_sems, local_sems,
):
    n_dp, n_t, length, feat, per_source = cfg
    chips = n_dp // CORES
    w_sub = feat // n_dp
    kd = k_in.shape[0]
    k_rows, k_cols = kd // chips, feat // CORES
    o_rows = o_in.shape[0]
    o_sub = o_rows // n_dp
    block = length // n_dp
    most = length // per_source
    rows = length // n_t
    qd = w_in.shape[1]
    heads = n_t * qd // HD
    half = length // 2
    me = lax.axis_index("dp")
    t = lax.axis_index("tensor")
    core = lax.rem(me, CORES)
    chip = lax.div(me, CORES)
    partner = chip * CORES + (CORES - 1 - core)
    near_x = chip + 1 - 2 * lax.rem(chip, SIDE)
    near_y = chip + SIDE - 2 * SIDE * lax.div(chip, SIDE)
    first_chip = near_x + core * (near_y - near_x)
    other_chip = near_y + core * (near_x - near_y)
    far_chip = chips - 1 - chip

    def t_at(k):
        return lax.rem(t + k, n_t)

    barrier = pltpu.get_barrier_semaphore()
    for k in range(1, n_dp):
        pl.semaphore_signal(
            barrier, inc=1, device_id=(lax.rem(me + k, n_dp), t), device_id_type=MESH
        )
    for k in range(1, n_t):
        pl.semaphore_signal(barrier, inc=1, device_id=(me, t_at(k)), device_id_type=MESH)

    small = [
        pltpu.make_async_copy(source, target, local_sems.at[4 + i])
        for i, (source, target) in enumerate(
            (
                (pk_hbm, pk_buf),
                (len_hbm, len_buf),
                (gain_hbm.at[:, pl.ds(aligned(t, feat), feat)], gain),
                (tab_hbm, tab),
            )
        )
    ]
    load = pltpu.make_async_copy(roll_hbm, roll_in, local_sems.at[2])
    own_w = pltpu.make_async_copy(
        w_in.at[pl.ds(aligned(t, feat), feat)], wbuf.at[t], local_sems.at[0]
    )
    own_k = pltpu.make_async_copy(
        k_in.at[:, pl.ds(aligned(t, feat), feat)],
        kbuf.at[pl.ds(aligned(t, kd), kd)],
        local_sems.at[3],
    )
    own_o = pltpu.make_async_copy(
        o_in.at[:, pl.ds(aligned(t, feat), feat)], obuf.at[t], local_sems.at[1]
    )
    for copy in [*small, load, own_k, own_w, own_o]:
        copy.start()

    started, named = [], []

    def slot():
        named.append(recv_sems.at[len(named)])
        return named[-1]

    def send(source, target, device, arrival):
        copy = pltpu.make_async_remote_copy(
            src_ref=source,
            dst_ref=target,
            send_sem=send_sem,
            recv_sem=arrival,
            device_id=device,
            device_id_type=MESH,
        )
        copy.start()
        started.append(copy)

    def arrived(ref, arrival):
        pltpu.make_async_copy(ref, ref, arrival).wait()

    def w_at(u, h, c):
        return wbuf.at[u, pl.ds(aligned(h * CORES + c, w_sub), w_sub)]

    def k_at(u, h, c):
        return kbuf.at[
            pl.ds(aligned(u * chips + h, k_rows), k_rows), pl.ds(aligned(c, k_cols), k_cols)
        ]

    def o_at(u, h, c):
        return obuf.at[u, pl.ds(aligned(h * CORES + c, o_sub), o_sub)]

    down = lax.broadcasted_iota(jnp.int32, (length, length), 0).astype(jnp.float32)
    across = lax.broadcasted_iota(jnp.int32, (length, length), 1).astype(jnp.float32)

    def part(value, size):
        return jnp.floor((value + 0.5) * (1.0 / size))

    def pick(mask, value, axis):
        return jnp.sum(jnp.where(mask, value, 0.0), axis=axis, keepdims=True)

    same = part(down, per_source) == part(across, per_source)
    diagonal = down == across
    for copy in small:
        copy.wait()
    len_all = len_buf[...].astype(jnp.float32)
    source_of = part(down[:, :1], per_source)
    table = jnp.zeros((length, per_source), jnp.float32)
    for i in range(n_dp):
        table = jnp.where(source_of == float(i), len_all[i : i + 1, :], table)
    within = down[:, :per_source] - source_of * per_source
    len_c = pick(across[:, :per_source] == within, table, 1)
    len_r = pick(diagonal, len_c, 0)
    pk_r = pk_buf[...].astype(jnp.float32)
    pk_c = pick(diagonal, pk_r, 1)
    src_start = pick(same & (across < down), len_r, 1)
    chosen = down == pk_r
    q_len_r = pick(chosen, len_c, 0)
    q_start_r = pick(chosen, src_start, 0)
    q_len_c = pick(across == pk_c, len_r, 1)
    earlier = same & (down < across)
    doc_start_r = pick(earlier, q_len_c, 0)
    q_src_r = part(pk_r, per_source)
    slot_r = pick(earlier & (part(pk_c, per_source) == q_src_r), 1.0, 0)
    mine = me.astype(jnp.float32)
    across_1 = across[:1]
    down_1 = down[:, :1]
    owner_r = part(across_1, per_source)
    target = jnp.where(q_src_r == mine, owner_r * (per_source // n_dp) + slot_r, -1.0)
    group = part(down_1, most)
    match = target == group
    token = down_1 - group * most
    row_sent = jnp.where(token < pick(match, q_len_r, 1), pick(match, q_start_r, 1) + token, -1.0)
    take_send = (across == row_sent).astype(jnp.float32).astype(jnp.bfloat16)

    tile = 256
    tiles = feat // tile
    load.wait()
    for i in range(tiles):
        at = slice(i * tile, (i + 1) * tile)
        sendb[:, at] = jnp.dot(
            take_send, roll_in[:, at], preferred_element_type=jnp.float32
        ).astype(jnp.bfloat16)

    pl.semaphore_wait(barrier, n_dp + n_t - 2)

    others = (1, 3, 2) if n_t == 4 else tuple(range(1, n_t))
    k_first = slot()
    for k in others:
        to = t_at(k)
        send(
            k_in.at[
                pl.ds(aligned(chip, k_rows), k_rows),
                pl.ds(aligned(to * CORES + core, k_cols), k_cols),
            ],
            k_at(t, chip, core),
            (me, to),
            k_first,
        )
    row_group = slot()

    def send_rows(to):
        send(
            sendb.at[pl.ds(aligned(to, block), block)],
            recvb.at[pl.ds(aligned(me, block), block)],
            (to, t),
            row_group,
        )

    for c in range(CORES):
        send_rows(far_chip * CORES + lax.rem(core + c, CORES))
    send_rows(partner)
    w_first = {k: slot() for k in others}
    o_first = {k: slot() for k in others}
    for k in others:
        to = t_at(k)
        send(
            w_in.at[pl.ds(aligned(to * n_dp + me, w_sub), w_sub)], w_at(t, chip, core), (me, to),
            w_first[k],
        )
    for k in others:
        to = t_at(k)
        send(
            o_in.at[pl.ds(aligned(me, o_sub), o_sub), pl.ds(aligned(to, feat), feat)],
            o_at(t, chip, core),
            (me, to),
            o_first[k],
        )

    keep = pl.ds(aligned(me, block), block)
    recvb[keep, :] = sendb[keep, :]
    inside = (owner_r == mine) & (doc_start_r <= down) & (down < doc_start_r + q_len_r)
    is_valid = pick(inside, 1.0, 1)
    position = (down_1 - pick(inside, doc_start_r, 1)) * is_valid
    row_got = jnp.where(
        is_valid > 0.0, pick(inside, q_src_r * block + slot_r * most, 1) + position, -1.0
    )
    take_recv = (across == row_got).astype(jnp.float32).astype(jnp.bfloat16)
    pos = jnp.broadcast_to(position, (length, HD))
    pos_buf[...] = pos
    valid_buf[...] = jnp.broadcast_to(is_valid, (length, HD))
    cosine = jnp.zeros((length, HD), jnp.float32)
    sine = jnp.zeros((length, HD), jnp.float32)
    for m in range(most):
        at_m = pos == float(m)
        cosine = jnp.where(at_m, tab[m : m + 1, :], cosine)
        sine = jnp.where(at_m, tab[most + m : most + m + 1, :], sine)
    cos_buf[...] = cosine
    sin_buf[...] = sine
    mask_buf[...] = ((across <= down) & (across >= down - position)).astype(jnp.float32)
    fold_down = lax.broadcasted_iota(jnp.int32, (length, HD), 0)
    fold_across = lax.broadcasted_iota(jnp.int32, (length, HD), 1)
    fold_buf[...] = (
        (lax.rem(fold_down, most) == lax.rem(fold_across, most))
        .astype(jnp.float32)
        .astype(jnp.bfloat16)
    )

    first_dev = first_chip * CORES + core
    other_dev = other_chip * CORES + core

    def spread(at, j, hops):
        ref = at(t_at(n_t - j), chip, core)
        send(ref, ref, (first_dev, t), hops[0])
        send(ref, ref, (other_dev, t), hops[1])
        send(ref, ref, (partner, t), hops[2])

    def relay(at, j, hops):
        ref = at(t_at(n_t - j), first_chip, core)
        send(ref, ref, (other_dev, t), hops[1])
        send(ref, ref, (partner, t), hops[2])

    def settle(at, j, hops):
        for source in (other_chip, far_chip):
            ref = at(t_at(n_t - j), source, core)
            send(ref, ref, (partner, t), hops[2])

    k_hops = [slot() for _ in range(3)]
    w_hops = {j: [slot() for _ in range(3)] for j in others}
    o_hops = {j: [slot() for _ in range(3)] for j in others}

    def k_wait(count, arrival):
        arrived(
            kbuf.at[pl.ds(0, count * k_rows), pl.ds(0, k_cols)], arrival
        )

    def w_wait(count, j, arrival):
        arrived(wbuf.at[t_at(n_t - j), pl.ds(0, count * w_sub)], arrival)

    def o_wait(count, j, arrival):
        arrived(obuf.at[t_at(n_t - j), pl.ds(0, count * o_sub)], arrival)

    def w_spread(j):
        w_wait(1, j, w_first[j])
        spread(w_at, j, w_hops[j])

    def w_relay(j):
        w_wait(1, j, w_hops[j][0])
        relay(w_at, j, w_hops[j])

    def w_settle(j):
        w_wait(2, j, w_hops[j][1])
        settle(w_at, j, w_hops[j])

    def o_spread(j):
        o_wait(1, j, o_first[j])
        spread(o_at, j, o_hops[j])

    def o_relay(j):
        o_wait(1, j, o_hops[j][0])
        relay(o_at, j, o_hops[j])

    def o_settle(j):
        o_wait(2, j, o_hops[j][1])
        settle(o_at, j, o_hops[j])

    one, three, two = others
    k_wait(n_t - 1, k_first)
    for j in others:
        spread(k_at, j, k_hops)
    for near in (first_chip, other_chip):
        for c in range(CORES):
            send_rows(near * CORES + lax.rem(core + c, CORES))
    k_wait(n_t - 1, k_hops[0])
    for j in others:
        relay(k_at, j, k_hops)
    w_spread(one)
    arrived(recvb.at[pl.ds(0, (n_dp - 1) * block)], row_group)
    w_spread(three)
    squares = jnp.zeros((length, 1), jnp.float32)
    for i in range(tiles):
        at = slice(i * tile, (i + 1) * tile)
        x = jnp.dot(take_recv, recvb[:, at], preferred_element_type=jnp.float32)
        packed[:, at] = x.astype(jnp.bfloat16)
        scaled[:, at] = (x * gain[:, at]).astype(jnp.bfloat16)
        squares += jnp.sum(x * x, axis=1, keepdims=True)
    sq_part[...] = jnp.broadcast_to(pick(diagonal, squares, 0), (8, length))
    sq_group = slot()
    for k in others:
        send(sq_part, sq_recv.at[k - 1], (me, t_at(k)), sq_group)
    w_spread(two)
    w_relay(one)
    k_wait(2 * (n_t - 1), k_hops[1])
    for j in others:
        settle(k_at, j, k_hops)
    own_k.wait()
    k_wait(chips * (n_t - 1), k_hops[2])
    kv_groups = [slot() for _ in range(2)]
    for c in range(2):
        cols = slice(c * HD, (c + 1) * HD)
        kv_part[:, cols] = lax.dot_general(
            scaled[...], kbuf[cols, :], (((1,), (1,)), ((), ())),
            preferred_element_type=jnp.float32,
        ).astype(jnp.bfloat16)
        for k in others:
            to = t_at(k)
            send(
                kv_part.at[pl.ds(aligned(to, rows), rows), cols],
                kv_recv.at[k - 1, :, cols],
                (me, to),
                kv_groups[c],
            )
    arrived(sq_recv, sq_group)
    sq = sq_part[:1, :]
    for k in range(n_t - 1):
        sq += sq_recv[k, :1, :]
    inverse = lax.rsqrt(sq / (feat * n_t) + epsilon)
    inv_buf[...] = jnp.broadcast_to(pick(diagonal, inverse, 1), (length, HD))

    def turn(v, c, s):
        return v * c + pltpu.roll(v, HD // 2, 1) * s

    def project(u):
        q = jnp.dot(scaled[...], wbuf[u], preferred_element_type=jnp.float32)
        for h in range(qd // HD):
            part_q = q[:, h * HD : (h + 1) * HD] * inv_buf[...]
            q_rot[:, pl.ds(aligned(u * (qd // HD) + h, HD), HD)] = turn(
                part_q, cos_buf[...], sin_buf[...]
            ).astype(jnp.bfloat16)

    own_w.wait()
    project(t)
    w_relay(three)
    w_relay(two)
    o_spread(one)
    o_spread(three)

    mine_rows = pl.ds(aligned(t, rows), rows)
    all_groups = [slot() for _ in range(2)]

    def share_kv(c):
        cols = slice(c * HD, (c + 1) * HD)
        arrived(kv_recv.at[:, :, cols], kv_groups[c])
        kv = kv_part[mine_rows, cols].astype(jnp.float32)
        for k in range(n_t - 1):
            kv += kv_recv[k, :, cols].astype(jnp.float32)
        kv = (kv * inv_buf[mine_rows, :]).astype(jnp.bfloat16)
        if c == 0:
            kv = turn(
                kv.astype(jnp.float32), cos_buf[mine_rows, :], sin_buf[mine_rows, :]
            ).astype(jnp.bfloat16)
        kv_all[mine_rows, cols] = kv
        at = kv_all.at[mine_rows, cols]
        for k in others:
            send(at, at, (me, t_at(k)), all_groups[c])

    share_kv(0)
    w_settle(one)
    w_wait(chips, one, w_hops[one][2])
    project(t_at(n_t - one))
    o_relay(one)
    share_kv(1)
    w_settle(three)
    w_wait(chips, three, w_hops[three][2])
    project(t_at(n_t - three))
    o_spread(two)
    w_settle(two)
    w_wait(chips, two, w_hops[two][2])
    project(t_at(n_t - two))
    o_relay(three)
    arrived(kv_all.at[pl.ds(0, (n_t - 1) * rows), pl.ds(0, HD)], all_groups[0])
    lane = lax.broadcasted_iota(jnp.int32, (half, HD), 1)
    line = lax.broadcasted_iota(jnp.int32, (half, HD), 0)
    cell = lax.div(lane, most)
    compact = jnp.zeros((half, HD), jnp.float32)
    for h in range(heads):
        scores = lax.dot_general(
            q_rot[:, h * HD : (h + 1) * HD], kv_all[:, :HD], (((1,), (1,)), ((), ())),
            preferred_element_type=jnp.float32,
        )
        scores = (scores * mask_buf[...]).astype(jnp.bfloat16)
        folded = jnp.dot(scores, fold_buf[...], preferred_element_type=jnp.float32)
        compact = jnp.where(cell == h, folded[:half], compact)
        compact = jnp.where(cell == heads + h, folded[half:], compact)
    score_part[...] = compact.astype(jnp.bfloat16)
    score_group = slot()
    for k in others:
        send(score_part, score_recv.at[k - 1], (me, t_at(k)), score_group)

    o_relay(two)
    for j in others:
        o_settle(j)

    arrived(score_recv, score_group)
    total = score_part[...].astype(jnp.float32)
    for k in range(n_t - 1):
        total += score_recv[k].astype(jnp.float32)
    place = jnp.where(cell < heads, pos_buf[:half, :], pos_buf[half:, :])
    back = lax.rem(line - lane + HD, most).astype(jnp.float32)
    total = jnp.where(back <= place, total * (1.0 / math.sqrt(HD)), -jnp.inf)

    def around(value, combine):
        step = 1
        while step < most:
            low = lax.rem(lax.div(lane, step), 2) == 0
            value = combine(
                value,
                jnp.where(low, pltpu.roll(value, HD - step, 1), pltpu.roll(value, step, 1)),
            )
            step *= 2
        return value

    exponent = jnp.exp(total - around(total, jnp.maximum))
    weights = exponent / around(exponent, jnp.add)
    arrived(kv_all.at[pl.ds(0, (n_t - 1) * rows), pl.ds(HD, HD)], all_groups[1])
    for h in range(heads):
        chosen_w = jnp.concatenate(
            [jnp.where(cell == h, weights, 0.0), jnp.where(cell == heads + h, weights, 0.0)], axis=0
        ).astype(jnp.bfloat16)
        dense = lax.dot_general(
            chosen_w, fold_buf[...], (((1,), (1,)), ((), ())), preferred_element_type=jnp.float32
        )
        dense = (dense * mask_buf[...]).astype(jnp.bfloat16)
        ctx[:, h * HD : (h + 1) * HD] = jnp.dot(
            dense, kv_all[:, HD:], preferred_element_type=jnp.float32
        ).astype(jnp.bfloat16)

    own_o.wait()
    for j in others:
        o_wait(chips, j, o_hops[j][2])

    for i in range(tiles):
        at = slice(i * tile, (i + 1) * tile)
        result = packed[:, at].astype(jnp.float32)
        for u in range(n_t):
            result += jnp.dot(
                ctx[:, u * o_rows : (u + 1) * o_rows],
                obuf[u, :, at],
                preferred_element_type=jnp.float32,
            )
        out[:, at] = jnp.where(valid_buf[:, :1] > 0.0, result, 0.0).astype(jnp.bfloat16)
    for copy in started:
        copy.wait_send()


def fused_body(rollout, lengths, packing, norm_gain, query_weight, keyval_weight, out_weight):
    n_dp, n_t = lax.axis_size("dp"), lax.axis_size("tensor")
    length, feat = rollout.shape
    per_source = lengths.shape[1]
    most = length // per_source
    qd, kd = query_weight.shape[1], keyval_weight.shape[1]
    frequency = np.float32(rope_base) ** (-np.arange(HD // 2, dtype=np.float32) * 2.0 / HD)
    angles = np.arange(most, dtype=np.float32)[:, None] * frequency[None, :].astype(np.float32)
    cos_tab = np.concatenate([np.cos(angles)] * 2, axis=1).astype(np.float32)
    sin_tab = np.concatenate([-np.sin(angles), np.sin(angles)], axis=1).astype(np.float32)
    rows = length // n_t
    groups = 4 + 8 * (n_t - 1) + 7
    vmem = pl.BlockSpec(memory_space=pltpu.VMEM)
    hbm = pl.BlockSpec(memory_space=pltpu.HBM)
    bf, f32 = jnp.bfloat16, jnp.float32
    return pl.pallas_call(
        functools.partial(fused_kernel, (n_dp, n_t, length, feat, per_source)),
        out_shape=jax.ShapeDtypeStruct((length, feat), bf),
        in_specs=[hbm] * 8,
        out_specs=vmem,
        scratch_shapes=[
            pltpu.VMEM((1, packing.shape[0]), jnp.int32),
            pltpu.VMEM(lengths.shape, jnp.int32),
            pltpu.VMEM((1, feat), f32),
            pltpu.VMEM((2 * most, HD), f32),
            pltpu.VMEM((n_t, feat, qd), bf),
            pltpu.VMEM((n_t * kd, feat), bf),
            pltpu.VMEM((n_t, out_weight.shape[0], feat), bf),
            pltpu.VMEM((length, feat), bf),
            pltpu.VMEM((length, feat), bf),
            pltpu.VMEM((length, feat), bf),
            pltpu.VMEM((length, feat), bf),
            pltpu.VMEM((length, feat), bf),
            pltpu.VMEM((length, n_t * qd), bf),
            pltpu.VMEM((length, 2 * HD), bf),
            pltpu.VMEM((n_t - 1, rows, 2 * HD), bf),
            pltpu.VMEM((length, 2 * HD), bf),
            pltpu.VMEM((length, n_t * qd), bf),
            pltpu.VMEM((length, HD), f32),
            pltpu.VMEM((length, HD), f32),
            pltpu.VMEM((length, HD), f32),
            pltpu.VMEM((length, HD), f32),
            pltpu.VMEM((length, HD), f32),
            pltpu.VMEM((length, length), f32),
            pltpu.VMEM((length, HD), bf),
            pltpu.VMEM((8, length), f32),
            pltpu.VMEM((n_t - 1, 8, length), f32),
            pltpu.VMEM((length // 2, HD), bf),
            pltpu.VMEM((n_t - 1, length // 2, HD), bf),
            pltpu.SemaphoreType.DMA,
            pltpu.SemaphoreType.DMA((groups,)),
            pltpu.SemaphoreType.DMA((8,)),
        ],
        compiler_params=pltpu.CompilerParams(
            collective_id=0, has_side_effects=True, vmem_limit_bytes=32 * 1024 * 1024
        ),
    )(
        *(
            pltpu.with_memory_space_constraint(operand, pltpu.HBM)
            for operand in (
                packing[None, :], lengths, norm_gain[None, :],
                jnp.asarray(np.concatenate([cos_tab, sin_tab])), rollout, query_weight,
                keyval_weight.T, out_weight,
            )
        )
    )


def body(rollout, lengths, packing, norm_gain, query_weight, keyval_weight, out_weight):
    n_dp, n_t = lax.axis_size("dp"), lax.axis_size("tensor")
    length, feat = rollout.shape
    per_source = lengths.shape[1]
    qd, kd = query_weight.shape[1], keyval_weight.shape[1]
    fits = (
        kd * n_t == 2 * HD
        and n_t == 4
        and n_dp == SIDE * SIDE * CORES
        and qd % HD == 0
        and n_t * qd // HD <= GROUP
        and per_source * 8 == length
        and n_t * qd // HD * 8 * 2 == HD
        and kd % (16 * n_dp // CORES) == 0
        and feat % (128 * CORES) == 0
        and length % (n_t * 16) == 0
        and length == 2 * HD
        and packing.shape[0] == length
        and (length // n_dp) % 16 == 0
        and feat % 512 == 0
        and per_source % n_dp == 0
    )
    chosen = fused_body if fits else plain_body
    return chosen(rollout, lengths, packing, norm_gain, query_weight, keyval_weight, out_weight)


def solution(mesh):
    in_specs = (
        P("dp", "tensor"),
        P(),
        P(),
        P(),
        P(None, "tensor"),
        P(None, "tensor"),
        P("tensor", None),
    )
    out_specs = P("dp", "tensor")
    return jax.shard_map(body, mesh=mesh, in_specs=in_specs, out_specs=out_specs, check_vma=False)
```

```python
import functools
import math

import numpy as np
import jax
import jax.numpy as jnp
from jax import lax
from jax.experimental import pallas as pl
from jax.experimental.pallas import tpu as pltpu
from jax.sharding import PartitionSpec as P

D = 6144
HD = 128
HQ_DEV = 2
GROUP = 8


epsilon = 1e-05
rope_base = 500000.0


def owner_map(lengths, packing, owner_id, pack_len):
    per_source = lengths.shape[1]
    chosen = lax.dynamic_slice_in_dim(packing, owner_id * per_source, per_source)
    ordered = jnp.take(lengths.reshape(-1), chosen)
    doc_start = jnp.cumsum(ordered) - ordered
    places = jnp.arange(pack_len, dtype=jnp.int32)
    inside = (places[:, None] >= doc_start[None, :]) & (
        places[:, None] < (doc_start + ordered)[None, :]
    )
    is_valid = jnp.any(inside, axis=1)
    slot_of = jnp.sum(
        jnp.where(inside, jnp.arange(per_source, dtype=jnp.int32)[None, :], 0), axis=1
    )
    response = jnp.take(chosen, slot_of)
    position = jnp.where(is_valid, places - jnp.take(doc_start, slot_of), 0)
    doc_id = jnp.where(is_valid, slot_of, per_source)
    return (response, position, doc_id, is_valid)


def rotate(values, position, head_dim):
    half_dim = head_dim // 2
    frequency = rope_base ** (-jnp.arange(half_dim, dtype=jnp.float32) * 2.0 / head_dim)
    angles = position.astype(jnp.float32)[:, None] * frequency[None, :]
    cosine = jnp.concatenate([jnp.cos(angles), jnp.cos(angles)], axis=1)[:, None, :]
    sine_table = jnp.concatenate([jnp.sin(angles), jnp.sin(angles)], axis=1)[:, None, :]
    turned = jnp.concatenate([-values[..., half_dim:], values[..., :half_dim]], axis=-1)
    return values * cosine + turned * sine_table


def plain_body(rollout, lengths, packing, norm_gain, query_weight, keyval_weight, out_weight):
    owner_id = lax.axis_index("dp")
    tensor_index = lax.axis_index("tensor")
    tensor_count = lax.axis_size("tensor")
    pack_len = rollout.shape[0]
    per_source = lengths.shape[1]
    response, position, doc_id, is_valid = owner_map(lengths, packing, owner_id, pack_len)
    source_start = jnp.cumsum(lengths, axis=1) - lengths
    global_row = (
        response // per_source * pack_len + jnp.take(source_start.reshape(-1), response) + position
    )
    portion = lax.all_gather(rollout, "dp", axis=0, tiled=True)
    within = is_valid & (global_row >= 0) & (global_row < portion.shape[0])
    picked = jnp.take(portion, jnp.clip(global_row, 0, portion.shape[0] - 1), axis=0)
    packed = jnp.where(within[:, None], picked, jnp.zeros_like(rollout))
    widened = lax.all_gather(packed, "tensor", axis=1, tiled=True).astype(jnp.float32)
    scaled = (widened * norm_gain[None, :]).astype(jnp.bfloat16)
    query_acc = jnp.dot(scaled, query_weight, preferred_element_type=jnp.float32)
    keyval_acc = jnp.dot(scaled, keyval_weight, preferred_element_type=jnp.float32)
    squares = jnp.sum(widened * widened, axis=1)
    query_acc, keyval_acc, squares = (query_acc, keyval_acc, squares)
    inverse = lax.rsqrt(squares / D + epsilon)
    queries = query_acc * inverse[:, None]
    keyval_share = (keyval_acc * inverse[:, None]).astype(jnp.bfloat16)
    keyval_all = lax.all_gather(keyval_share, "tensor", axis=1, tiled=True)
    kv_count = keyval_weight.shape[1] * tensor_count // (2 * HD)
    shared_head = tensor_index * HQ_DEV // GROUP
    keys = lax.dynamic_slice_in_dim(keyval_all, shared_head * HD, HD, 1)
    values = lax.dynamic_slice_in_dim(keyval_all, (kv_count + shared_head) * HD, HD, 1)
    q_rot = rotate(queries.reshape(pack_len, HQ_DEV, HD), position, HD).astype(jnp.bfloat16)
    k_rot = rotate(keys.astype(jnp.float32)[:, None, :], position, HD)[:, 0, :].astype(jnp.bfloat16)
    scores = jnp.einsum(
        "qhd,kd->hqk", q_rot, k_rot, preferred_element_type=jnp.float32
    ) / math.sqrt(HD)
    places = jnp.arange(pack_len, dtype=jnp.int32)
    allowed = (doc_id[:, None] == doc_id[None, :]) & (places[None, :] <= places[:, None])
    masked = jnp.where(allowed[None], scores, -jnp.inf)
    row_max = jnp.max(masked, axis=2, keepdims=True)
    exponent = jnp.exp(masked - row_max)
    weights = (exponent / jnp.sum(exponent, axis=2, keepdims=True)).astype(jnp.bfloat16)
    context = jnp.einsum("hqk,kd->qhd", weights, values, preferred_element_type=jnp.float32)
    context = context.astype(jnp.bfloat16).reshape(pack_len, HQ_DEV * HD)
    partial_sum = jnp.dot(context, out_weight, preferred_element_type=jnp.float32)
    summed = lax.psum_scatter(
        partial_sum.astype(jnp.bfloat16), "tensor", scatter_dimension=1, tiled=True
    ).astype(jnp.float32)
    result = jnp.where(is_valid[:, None], summed + packed.astype(jnp.float32), 0.0)
    return result.astype(jnp.bfloat16)


MESH = pl.DeviceIdType.MESH
CORES = 2
SIDE = 2


def aligned(index, size):
    return pl.multiple_of(index * size, size)


def fused_kernel(
    cfg, pk_hbm, len_hbm, gain_hbm, tab_hbm, roll_hbm, w_in, k_in, o_in, out,
    pk_buf, len_buf, gain, tab, wbuf, kbuf, obuf, roll_in, sendb, recvb, packed, scaled, q_rot, kv_part, kv_recv, kv_all, ctx,
    pos_buf, valid_buf, cos_buf, sin_buf, inv_buf, mask_buf, fold_buf, sq_part, sq_recv, score_part, score_recv,
    send_sem, recv_sems, local_sems,
):
    n_dp, n_t, length, feat, per_source = cfg
    chips = n_dp // CORES
    w_sub = feat // n_dp
    kd = k_in.shape[0]
    k_rows, k_cols = kd // chips, feat // CORES
    o_rows = o_in.shape[0]
    o_sub = o_rows // n_dp
    block = length // n_dp
    most = length // per_source
    rows = length // n_t
    qd = w_in.shape[1]
    heads = n_t * qd // HD
    half = length // 2
    me = lax.axis_index("dp")
    t = lax.axis_index("tensor")
    core = lax.rem(me, CORES)
    chip = lax.div(me, CORES)
    partner = chip * CORES + (CORES - 1 - core)
    near_x = chip + 1 - 2 * lax.rem(chip, SIDE)
    near_y = chip + SIDE - 2 * SIDE * lax.div(chip, SIDE)
    first_chip = near_x + core * (near_y - near_x)
    other_chip = near_y + core * (near_x - near_y)
    far_chip = chips - 1 - chip

    def t_at(k):
        return lax.rem(t + k, n_t)

    barrier = pltpu.get_barrier_semaphore()
    for k in range(1, n_dp):
        pl.semaphore_signal(
            barrier, inc=1, device_id=(lax.rem(me + k, n_dp), t), device_id_type=MESH
        )
    for k in range(1, n_t):
        pl.semaphore_signal(barrier, inc=1, device_id=(me, t_at(k)), device_id_type=MESH)

    small = [
        pltpu.make_async_copy(source, target, local_sems.at[4 + i])
        for i, (source, target) in enumerate(
            (
                (pk_hbm, pk_buf),
                (len_hbm, len_buf),
                (gain_hbm.at[:, pl.ds(aligned(t, feat), feat)], gain),
                (tab_hbm, tab),
            )
        )
    ]
    load = pltpu.make_async_copy(roll_hbm, roll_in, local_sems.at[2])
    own_w = pltpu.make_async_copy(
        w_in.at[pl.ds(aligned(t, feat), feat)], wbuf.at[t], local_sems.at[0]
    )
    own_k = pltpu.make_async_copy(
        k_in.at[:, pl.ds(aligned(t, feat), feat)],
        kbuf.at[pl.ds(aligned(t, kd), kd)],
        local_sems.at[3],
    )
    own_o = pltpu.make_async_copy(
        o_in.at[:, pl.ds(aligned(t, feat), feat)], obuf.at[t], local_sems.at[1]
    )
    for copy in [*small, load, own_k, own_w, own_o]:
        copy.start()

    started, named = [], []

    def slot():
        named.append(recv_sems.at[len(named)])
        return named[-1]

    def send(source, target, device, arrival):
        copy = pltpu.make_async_remote_copy(
            src_ref=source,
            dst_ref=target,
            send_sem=send_sem,
            recv_sem=arrival,
            device_id=device,
            device_id_type=MESH,
        )
        copy.start()
        started.append(copy)

    def arrived(ref, arrival):
        pltpu.make_async_copy(ref, ref, arrival).wait()

    def w_at(u, h, c):
        return wbuf.at[u, pl.ds(aligned(h * CORES + c, w_sub), w_sub)]

    def k_at(u, h, c):
        return kbuf.at[
            pl.ds(aligned(u * chips + h, k_rows), k_rows), pl.ds(aligned(c, k_cols), k_cols)
        ]

    def o_at(u, h, c):
        return obuf.at[u, pl.ds(aligned(h * CORES + c, o_sub), o_sub)]

    down = lax.broadcasted_iota(jnp.int32, (length, length), 0).astype(jnp.float32)
    across = lax.broadcasted_iota(jnp.int32, (length, length), 1).astype(jnp.float32)

    def part(value, size):
        return jnp.floor((value + 0.5) * (1.0 / size))

    def pick(mask, value, axis):
        return jnp.sum(jnp.where(mask, value, 0.0), axis=axis, keepdims=True)

    same = part(down, per_source) == part(across, per_source)
    diagonal = down == across
    for copy in small:
        copy.wait()
    len_all = len_buf[...].astype(jnp.float32)
    source_of = part(down[:, :1], per_source)
    table = jnp.zeros((length, per_source), jnp.float32)
    for i in range(n_dp):
        table = jnp.where(source_of == float(i), len_all[i : i + 1, :], table)
    within = down[:, :per_source] - source_of * per_source
    len_c = pick(across[:, :per_source] == within, table, 1)
    len_r = pick(diagonal, len_c, 0)
    pk_r = pk_buf[...].astype(jnp.float32)
    pk_c = pick(diagonal, pk_r, 1)
    src_start = pick(same & (across < down), len_r, 1)
    chosen = down == pk_r
    q_len_r = pick(chosen, len_c, 0)
    q_start_r = pick(chosen, src_start, 0)
    q_len_c = pick(across == pk_c, len_r, 1)
    earlier = same & (down < across)
    doc_start_r = pick(earlier, q_len_c, 0)
    q_src_r = part(pk_r, per_source)
    slot_r = pick(earlier & (part(pk_c, per_source) == q_src_r), 1.0, 0)
    mine = me.astype(jnp.float32)
    across_1 = across[:1]
    down_1 = down[:, :1]
    owner_r = part(across_1, per_source)
    target = jnp.where(q_src_r == mine, owner_r * (per_source // n_dp) + slot_r, -1.0)
    group = part(down_1, most)
    match = target == group
    token = down_1 - group * most
    row_sent = jnp.where(token < pick(match, q_len_r, 1), pick(match, q_start_r, 1) + token, -1.0)
    take_send = (across == row_sent).astype(jnp.float32).astype(jnp.bfloat16)

    tile = 256
    tiles = feat // tile
    load.wait()
    for i in range(tiles):
        at = slice(i * tile, (i + 1) * tile)
        sendb[:, at] = jnp.dot(
            take_send, roll_in[:, at], preferred_element_type=jnp.float32
        ).astype(jnp.bfloat16)

    pl.semaphore_wait(barrier, n_dp + n_t - 2)

    others = (1, 3, 2) if n_t == 4 else tuple(range(1, n_t))
    k_first = slot()
    for k in others:
        to = t_at(k)
        send(
            k_in.at[
                pl.ds(aligned(chip, k_rows), k_rows),
                pl.ds(aligned(to * CORES + core, k_cols), k_cols),
            ],
            k_at(t, chip, core),
            (me, to),
            k_first,
        )
    row_group = slot()

    def send_rows(to):
        send(
            sendb.at[pl.ds(aligned(to, block), block)],
            recvb.at[pl.ds(aligned(me, block), block)],
            (to, t),
            row_group,
        )

    for c in range(CORES):
        send_rows(far_chip * CORES + lax.rem(core + c, CORES))
    for c in range(CORES):
        send_rows(first_chip * CORES + lax.rem(core + c, CORES))
    send_rows(partner)
    w_first = {k: slot() for k in others}
    o_first = {k: slot() for k in others}

    def send_w(k):
        to = t_at(k)
        send(
            w_in.at[pl.ds(aligned(to * n_dp + me, w_sub), w_sub)], w_at(t, chip, core), (me, to),
            w_first[k],
        )

    send_w(1)

    def send_o(k):
        to = t_at(k)
        send(
            o_in.at[pl.ds(aligned(me, o_sub), o_sub), pl.ds(aligned(to, feat), feat)],
            o_at(t, chip, core),
            (me, to),
            o_first[k],
        )

    keep = pl.ds(aligned(me, block), block)
    recvb[keep, :] = sendb[keep, :]
    inside = (owner_r == mine) & (doc_start_r <= down) & (down < doc_start_r + q_len_r)
    is_valid = pick(inside, 1.0, 1)
    position = (down_1 - pick(inside, doc_start_r, 1)) * is_valid
    row_got = jnp.where(
        is_valid > 0.0, pick(inside, q_src_r * block + slot_r * most, 1) + position, -1.0
    )
    take_recv = (across == row_got).astype(jnp.float32).astype(jnp.bfloat16)
    pos = jnp.broadcast_to(position, (length, HD))
    pos_buf[...] = pos
    valid_buf[...] = jnp.broadcast_to(is_valid, (length, HD))
    cosine = jnp.zeros((length, HD), jnp.float32)
    sine = jnp.zeros((length, HD), jnp.float32)
    for m in range(most):
        at_m = pos == float(m)
        cosine = jnp.where(at_m, tab[m : m + 1, :], cosine)
        sine = jnp.where(at_m, tab[most + m : most + m + 1, :], sine)
    cos_buf[...] = cosine
    sin_buf[...] = sine
    mask_buf[...] = ((across <= down) & (across >= down - position)).astype(jnp.float32)
    fold_down = lax.broadcasted_iota(jnp.int32, (length, HD), 0)
    fold_across = lax.broadcasted_iota(jnp.int32, (length, HD), 1)
    fold_buf[...] = (
        (lax.rem(fold_down, most) == lax.rem(fold_across, most))
        .astype(jnp.float32)
        .astype(jnp.bfloat16)
    )

    first_dev = first_chip * CORES + core
    other_dev = other_chip * CORES + core

    def spread(at, j, hops):
        ref = at(t_at(n_t - j), chip, core)
        send(ref, ref, (first_dev, t), hops[0])
        send(ref, ref, (other_dev, t), hops[1])
        send(ref, ref, (partner, t), hops[2])

    def relay(at, j, hops):
        ref = at(t_at(n_t - j), first_chip, core)
        send(ref, ref, (other_dev, t), hops[1])
        send(ref, ref, (partner, t), hops[2])

    def settle(at, j, hops):
        for source in (other_chip, far_chip):
            ref = at(t_at(n_t - j), source, core)
            send(ref, ref, (partner, t), hops[2])

    k_hops = [slot() for _ in range(3)]
    w_hops = {j: [slot() for _ in range(3)] for j in others}
    o_hops = {j: [slot() for _ in range(3)] for j in others}

    def k_wait(count, arrival):
        arrived(
            kbuf.at[pl.ds(0, count * k_rows), pl.ds(0, k_cols)], arrival
        )

    def w_wait(count, j, arrival):
        arrived(wbuf.at[t_at(n_t - j), pl.ds(0, count * w_sub)], arrival)

    def o_wait(count, j, arrival):
        arrived(obuf.at[t_at(n_t - j), pl.ds(0, count * o_sub)], arrival)

    def w_spread(j):
        w_wait(1, j, w_first[j])
        spread(w_at, j, w_hops[j])

    def w_relay(j):
        w_wait(1, j, w_hops[j][0])
        relay(w_at, j, w_hops[j])

    def w_settle(j):
        w_wait(2, j, w_hops[j][1])
        settle(w_at, j, w_hops[j])

    def o_spread(j):
        o_wait(1, j, o_first[j])
        spread(o_at, j, o_hops[j])

    def o_relay(j):
        o_wait(1, j, o_hops[j][0])
        relay(o_at, j, o_hops[j])

    def o_settle(j):
        o_wait(2, j, o_hops[j][1])
        settle(o_at, j, o_hops[j])

    one, three, two = others
    o_early, o_late = (one, three), (two,)
    o_a, o_b, o_c = o_early + o_late
    k_wait(n_t - 1, k_first)
    for j in others:
        spread(k_at, j, k_hops)
    for c in range(CORES):
        send_rows(other_chip * CORES + lax.rem(core + c, CORES))
    send_w(three)
    send_w(two)
    w_spread(one)
    send_o(one)
    k_wait(n_t - 1, k_hops[0])
    for j in others:
        relay(k_at, j, k_hops)
    arrived(recvb.at[pl.ds(0, (n_dp - 1) * block)], row_group)
    w_spread(three)
    squares = jnp.zeros((length, 1), jnp.float32)
    for i in range(tiles):
        at = slice(i * tile, (i + 1) * tile)
        x = jnp.dot(take_recv, recvb[:, at], preferred_element_type=jnp.float32)
        packed[:, at] = x.astype(jnp.bfloat16)
        scaled[:, at] = (x * gain[:, at]).astype(jnp.bfloat16)
        squares += jnp.sum(x * x, axis=1, keepdims=True)
    sq_part[...] = jnp.broadcast_to(pick(diagonal, squares, 0), (8, length))
    sq_group = slot()
    for k in others:
        send(sq_part, sq_recv.at[k - 1], (me, t_at(k)), sq_group)
    send_o(three)
    w_spread(two)
    w_relay(one)
    k_wait(2 * (n_t - 1), k_hops[1])
    for j in others:
        settle(k_at, j, k_hops)
    own_k.wait()
    k_wait(chips * (n_t - 1), k_hops[2])
    kv_groups = [slot() for _ in range(2)]
    for c in range(2):
        cols = slice(c * HD, (c + 1) * HD)
        kv_part[:, cols] = lax.dot_general(
            scaled[...], kbuf[cols, :], (((1,), (1,)), ((), ())),
            preferred_element_type=jnp.float32,
        ).astype(jnp.bfloat16)
        for k in others:
            to = t_at(k)
            send(
                kv_part.at[pl.ds(aligned(to, rows), rows), cols],
                kv_recv.at[k - 1, :, cols],
                (me, to),
                kv_groups[c],
            )
        if c == 0:
            send_o(two)
    w_relay(three)
    arrived(sq_recv, sq_group)
    sq = sq_part[:1, :]
    for k in range(n_t - 1):
        sq += sq_recv[k, :1, :]
    inverse = lax.rsqrt(sq / (feat * n_t) + epsilon)
    inv_buf[...] = jnp.broadcast_to(pick(diagonal, inverse, 1), (length, HD))

    def turn(v, c, s):
        return v * c + pltpu.roll(v, HD // 2, 1) * s

    def project(u):
        q = jnp.dot(scaled[...], wbuf[u], preferred_element_type=jnp.float32)
        for h in range(qd // HD):
            part_q = q[:, h * HD : (h + 1) * HD] * inv_buf[...]
            q_rot[:, pl.ds(aligned(u * (qd // HD) + h, HD), HD)] = turn(
                part_q, cos_buf[...], sin_buf[...]
            ).astype(jnp.bfloat16)

    own_w.wait()
    project(t)
    mine_rows = pl.ds(aligned(t, rows), rows)
    all_groups = [slot() for _ in range(2)]

    def share_kv(c):
        cols = slice(c * HD, (c + 1) * HD)
        arrived(kv_recv.at[:, :, cols], kv_groups[c])
        kv = kv_part[mine_rows, cols].astype(jnp.float32)
        for k in range(n_t - 1):
            kv += kv_recv[k, :, cols].astype(jnp.float32)
        kv = (kv * inv_buf[mine_rows, :]).astype(jnp.bfloat16)
        if c == 0:
            kv = turn(
                kv.astype(jnp.float32), cos_buf[mine_rows, :], sin_buf[mine_rows, :]
            ).astype(jnp.bfloat16)
        kv_all[mine_rows, cols] = kv
        at = kv_all.at[mine_rows, cols]
        for k in others:
            send(at, at, (me, t_at(k)), all_groups[c])

    w_relay(two)
    w_settle(one)
    share_kv(0)
    w_settle(three)
    o_spread(o_a)
    w_wait(chips, one, w_hops[one][2])
    project(t_at(n_t - one))
    w_settle(two)
    o_spread(o_b)
    w_wait(chips, three, w_hops[three][2])
    project(t_at(n_t - three))
    w_wait(chips, two, w_hops[two][2])
    project(t_at(n_t - two))
    share_kv(1)
    o_relay(o_a)
    o_spread(o_c)
    arrived(kv_all.at[pl.ds(0, (n_t - 1) * rows), pl.ds(0, HD)], all_groups[0])
    lane = lax.broadcasted_iota(jnp.int32, (half, HD), 1)
    line = lax.broadcasted_iota(jnp.int32, (half, HD), 0)
    cell = lax.div(lane, most)
    compact = jnp.zeros((half, HD), jnp.float32)
    for h in range(heads):
        scores = lax.dot_general(
            q_rot[:, h * HD : (h + 1) * HD], kv_all[:, :HD], (((1,), (1,)), ((), ())),
            preferred_element_type=jnp.float32,
        )
        scores = (scores * mask_buf[...]).astype(jnp.bfloat16)
        folded = jnp.dot(scores, fold_buf[...], preferred_element_type=jnp.float32)
        compact = jnp.where(cell == h, folded[:half], compact)
        compact = jnp.where(cell == heads + h, folded[half:], compact)
    score_part[...] = compact.astype(jnp.bfloat16)
    score_group = slot()
    for k in others:
        send(score_part, score_recv.at[k - 1], (me, t_at(k)), score_group)

    o_relay(o_b)
    o_settle(o_a)
    o_relay(o_c)
    o_settle(o_b)
    o_settle(o_c)
    arrived(score_recv, score_group)
    total = score_part[...].astype(jnp.float32)
    for k in range(n_t - 1):
        total += score_recv[k].astype(jnp.float32)
    place = jnp.where(cell < heads, pos_buf[:half, :], pos_buf[half:, :])
    back = lax.rem(line - lane + HD, most).astype(jnp.float32)
    total = jnp.where(back <= place, total * (1.0 / math.sqrt(HD)), -jnp.inf)

    def around(value, combine):
        step = 1
        while step < most:
            low = lax.rem(lax.div(lane, step), 2) == 0
            value = combine(
                value,
                jnp.where(low, pltpu.roll(value, HD - step, 1), pltpu.roll(value, step, 1)),
            )
            step *= 2
        return value

    exponent = jnp.exp(total - around(total, jnp.maximum))
    weights = exponent / around(exponent, jnp.add)
    arrived(kv_all.at[pl.ds(0, (n_t - 1) * rows), pl.ds(HD, HD)], all_groups[1])
    for h in range(heads):
        chosen_w = jnp.concatenate(
            [jnp.where(cell == h, weights, 0.0), jnp.where(cell == heads + h, weights, 0.0)], axis=0
        ).astype(jnp.bfloat16)
        dense = lax.dot_general(
            chosen_w, fold_buf[...], (((1,), (1,)), ((), ())), preferred_element_type=jnp.float32
        )
        dense = (dense * mask_buf[...]).astype(jnp.bfloat16)
        ctx[:, h * HD : (h + 1) * HD] = jnp.dot(
            dense, kv_all[:, HD:], preferred_element_type=jnp.float32
        ).astype(jnp.bfloat16)

    own_o.wait()
    for j in others:
        o_wait(chips, j, o_hops[j][2])

    for i in range(tiles):
        at = slice(i * tile, (i + 1) * tile)
        result = packed[:, at].astype(jnp.float32)
        for u in range(n_t):
            result += jnp.dot(
                ctx[:, u * o_rows : (u + 1) * o_rows],
                obuf[u, :, at],
                preferred_element_type=jnp.float32,
            )
        out[:, at] = jnp.where(valid_buf[:, :1] > 0.0, result, 0.0).astype(jnp.bfloat16)
    for copy in started:
        copy.wait_send()


def fused_body(rollout, lengths, packing, norm_gain, query_weight, keyval_weight, out_weight):
    n_dp, n_t = lax.axis_size("dp"), lax.axis_size("tensor")
    length, feat = rollout.shape
    per_source = lengths.shape[1]
    most = length // per_source
    qd, kd = query_weight.shape[1], keyval_weight.shape[1]
    frequency = np.float32(rope_base) ** (-np.arange(HD // 2, dtype=np.float32) * 2.0 / HD)
    angles = np.arange(most, dtype=np.float32)[:, None] * frequency[None, :].astype(np.float32)
    cos_tab = np.concatenate([np.cos(angles)] * 2, axis=1).astype(np.float32)
    sin_tab = np.concatenate([-np.sin(angles), np.sin(angles)], axis=1).astype(np.float32)
    rows = length // n_t
    groups = 4 + 8 * (n_t - 1) + 7
    vmem = pl.BlockSpec(memory_space=pltpu.VMEM)
    hbm = pl.BlockSpec(memory_space=pltpu.HBM)
    bf, f32 = jnp.bfloat16, jnp.float32
    return pl.pallas_call(
        functools.partial(fused_kernel, (n_dp, n_t, length, feat, per_source)),
        out_shape=jax.ShapeDtypeStruct((length, feat), bf),
        in_specs=[hbm] * 8,
        out_specs=vmem,
        scratch_shapes=[
            pltpu.VMEM((1, packing.shape[0]), jnp.int32),
            pltpu.VMEM(lengths.shape, jnp.int32),
            pltpu.VMEM((1, feat), f32),
            pltpu.VMEM((2 * most, HD), f32),
            pltpu.VMEM((n_t, feat, qd), bf),
            pltpu.VMEM((n_t * kd, feat), bf),
            pltpu.VMEM((n_t, out_weight.shape[0], feat), bf),
            pltpu.VMEM((length, feat), bf),
            pltpu.VMEM((length, feat), bf),
            pltpu.VMEM((length, feat), bf),
            pltpu.VMEM((length, feat), bf),
            pltpu.VMEM((length, feat), bf),
            pltpu.VMEM((length, n_t * qd), bf),
            pltpu.VMEM((length, 2 * HD), bf),
            pltpu.VMEM((n_t - 1, rows, 2 * HD), bf),
            pltpu.VMEM((length, 2 * HD), bf),
            pltpu.VMEM((length, n_t * qd), bf),
            pltpu.VMEM((length, HD), f32),
            pltpu.VMEM((length, HD), f32),
            pltpu.VMEM((length, HD), f32),
            pltpu.VMEM((length, HD), f32),
            pltpu.VMEM((length, HD), f32),
            pltpu.VMEM((length, length), f32),
            pltpu.VMEM((length, HD), bf),
            pltpu.VMEM((8, length), f32),
            pltpu.VMEM((n_t - 1, 8, length), f32),
            pltpu.VMEM((length // 2, HD), bf),
            pltpu.VMEM((n_t - 1, length // 2, HD), bf),
            pltpu.SemaphoreType.DMA,
            pltpu.SemaphoreType.DMA((groups,)),
            pltpu.SemaphoreType.DMA((8,)),
        ],
        compiler_params=pltpu.CompilerParams(
            collective_id=0, has_side_effects=True, vmem_limit_bytes=32 * 1024 * 1024
        ),
    )(
        *(
            pltpu.with_memory_space_constraint(operand, pltpu.HBM)
            for operand in (
                packing[None, :], lengths, norm_gain[None, :],
                jnp.asarray(np.concatenate([cos_tab, sin_tab])), rollout, query_weight,
                keyval_weight.T, out_weight,
            )
        )
    )


def body(rollout, lengths, packing, norm_gain, query_weight, keyval_weight, out_weight):
    n_dp, n_t = lax.axis_size("dp"), lax.axis_size("tensor")
    length, feat = rollout.shape
    per_source = lengths.shape[1]
    qd, kd = query_weight.shape[1], keyval_weight.shape[1]
    fits = (
        kd * n_t == 2 * HD
        and n_t == 4
        and n_dp == SIDE * SIDE * CORES
        and qd % HD == 0
        and n_t * qd // HD <= GROUP
        and per_source * 8 == length
        and n_t * qd // HD * 8 * 2 == HD
        and kd % (16 * n_dp // CORES) == 0
        and feat % (128 * CORES) == 0
        and length % (n_t * 16) == 0
        and length == 2 * HD
        and packing.shape[0] == length
        and (length // n_dp) % 16 == 0
        and feat % 512 == 0
        and per_source % n_dp == 0
    )
    chosen = fused_body if fits else plain_body
    return chosen(rollout, lengths, packing, norm_gain, query_weight, keyval_weight, out_weight)


def solution(mesh):
    in_specs = (
        P("dp", "tensor"),
        P(),
        P(),
        P(),
        P(None, "tensor"),
        P(None, "tensor"),
        P("tensor", None),
    )
    out_specs = P("dp", "tensor")
    return jax.shard_map(body, mesh=mesh, in_specs=in_specs, out_specs=out_specs, check_vma=False)
```

```python
import functools
import math

import numpy as np
import jax
import jax.numpy as jnp
from jax import lax
from jax.experimental import pallas as pl
from jax.experimental.pallas import tpu as pltpu
from jax.sharding import PartitionSpec as P

D = 6144
HD = 128
HQ_DEV = 2
GROUP = 8


epsilon = 1e-05
rope_base = 500000.0


def owner_map(lengths, packing, owner_id, pack_len):
    per_source = lengths.shape[1]
    chosen = lax.dynamic_slice_in_dim(packing, owner_id * per_source, per_source)
    ordered = jnp.take(lengths.reshape(-1), chosen)
    doc_start = jnp.cumsum(ordered) - ordered
    places = jnp.arange(pack_len, dtype=jnp.int32)
    inside = (places[:, None] >= doc_start[None, :]) & (
        places[:, None] < (doc_start + ordered)[None, :]
    )
    is_valid = jnp.any(inside, axis=1)
    slot_of = jnp.sum(
        jnp.where(inside, jnp.arange(per_source, dtype=jnp.int32)[None, :], 0), axis=1
    )
    response = jnp.take(chosen, slot_of)
    position = jnp.where(is_valid, places - jnp.take(doc_start, slot_of), 0)
    doc_id = jnp.where(is_valid, slot_of, per_source)
    return (response, position, doc_id, is_valid)


def rotate(values, position, head_dim):
    half_dim = head_dim // 2
    frequency = rope_base ** (-jnp.arange(half_dim, dtype=jnp.float32) * 2.0 / head_dim)
    angles = position.astype(jnp.float32)[:, None] * frequency[None, :]
    cosine = jnp.concatenate([jnp.cos(angles), jnp.cos(angles)], axis=1)[:, None, :]
    sine_table = jnp.concatenate([jnp.sin(angles), jnp.sin(angles)], axis=1)[:, None, :]
    turned = jnp.concatenate([-values[..., half_dim:], values[..., :half_dim]], axis=-1)
    return values * cosine + turned * sine_table


def plain_body(rollout, lengths, packing, norm_gain, query_weight, keyval_weight, out_weight):
    owner_id = lax.axis_index("dp")
    tensor_index = lax.axis_index("tensor")
    tensor_count = lax.axis_size("tensor")
    pack_len = rollout.shape[0]
    per_source = lengths.shape[1]
    response, position, doc_id, is_valid = owner_map(lengths, packing, owner_id, pack_len)
    source_start = jnp.cumsum(lengths, axis=1) - lengths
    global_row = (
        response // per_source * pack_len + jnp.take(source_start.reshape(-1), response) + position
    )
    portion = lax.all_gather(rollout, "dp", axis=0, tiled=True)
    within = is_valid & (global_row >= 0) & (global_row < portion.shape[0])
    picked = jnp.take(portion, jnp.clip(global_row, 0, portion.shape[0] - 1), axis=0)
    packed = jnp.where(within[:, None], picked, jnp.zeros_like(rollout))
    widened = lax.all_gather(packed, "tensor", axis=1, tiled=True).astype(jnp.float32)
    scaled = (widened * norm_gain[None, :]).astype(jnp.bfloat16)
    query_acc = jnp.dot(scaled, query_weight, preferred_element_type=jnp.float32)
    keyval_acc = jnp.dot(scaled, keyval_weight, preferred_element_type=jnp.float32)
    squares = jnp.sum(widened * widened, axis=1)
    query_acc, keyval_acc, squares = (query_acc, keyval_acc, squares)
    inverse = lax.rsqrt(squares / D + epsilon)
    queries = query_acc * inverse[:, None]
    keyval_share = (keyval_acc * inverse[:, None]).astype(jnp.bfloat16)
    keyval_all = lax.all_gather(keyval_share, "tensor", axis=1, tiled=True)
    kv_count = keyval_weight.shape[1] * tensor_count // (2 * HD)
    shared_head = tensor_index * HQ_DEV // GROUP
    keys = lax.dynamic_slice_in_dim(keyval_all, shared_head * HD, HD, 1)
    values = lax.dynamic_slice_in_dim(keyval_all, (kv_count + shared_head) * HD, HD, 1)
    q_rot = rotate(queries.reshape(pack_len, HQ_DEV, HD), position, HD).astype(jnp.bfloat16)
    k_rot = rotate(keys.astype(jnp.float32)[:, None, :], position, HD)[:, 0, :].astype(jnp.bfloat16)
    scores = jnp.einsum(
        "qhd,kd->hqk", q_rot, k_rot, preferred_element_type=jnp.float32
    ) / math.sqrt(HD)
    places = jnp.arange(pack_len, dtype=jnp.int32)
    allowed = (doc_id[:, None] == doc_id[None, :]) & (places[None, :] <= places[:, None])
    masked = jnp.where(allowed[None], scores, -jnp.inf)
    row_max = jnp.max(masked, axis=2, keepdims=True)
    exponent = jnp.exp(masked - row_max)
    weights = (exponent / jnp.sum(exponent, axis=2, keepdims=True)).astype(jnp.bfloat16)
    context = jnp.einsum("hqk,kd->qhd", weights, values, preferred_element_type=jnp.float32)
    context = context.astype(jnp.bfloat16).reshape(pack_len, HQ_DEV * HD)
    partial_sum = jnp.dot(context, out_weight, preferred_element_type=jnp.float32)
    summed = lax.psum_scatter(
        partial_sum.astype(jnp.bfloat16), "tensor", scatter_dimension=1, tiled=True
    ).astype(jnp.float32)
    result = jnp.where(is_valid[:, None], summed + packed.astype(jnp.float32), 0.0)
    return result.astype(jnp.bfloat16)


MESH = pl.DeviceIdType.MESH
CORES = 2
SIDE = 2


def aligned(index, size):
    return pl.multiple_of(index * size, size)


def fused_kernel(
    cfg, pk_hbm, len_hbm, gain_hbm, tab_hbm, roll_hbm, w_in, k_in, o_in, out,
    pk_buf, len_buf, gain, tab, wbuf, kbuf, obuf, roll_in, sendb, recvb, packed, scaled, q_rot, kv_part, kv_recv, kv_all, ctx,
    pos_buf, valid_buf, cos_buf, sin_buf, inv_buf, mask_buf, fold_buf, sq_part, sq_recv, score_part, score_recv, acc,
    send_sem, recv_sems, local_sems,
):
    n_dp, n_t, length, feat, per_source = cfg
    chips = n_dp // CORES
    w_sub = feat // n_dp
    kd = k_in.shape[0]
    k_rows, k_cols = kd // chips, feat // CORES
    o_rows = o_in.shape[0]
    o_sub = o_rows // n_dp
    block = length // n_dp
    most = length // per_source
    rows = length // n_t
    qd = w_in.shape[1]
    heads = n_t * qd // HD
    half = length // 2
    me = lax.axis_index("dp")
    t = lax.axis_index("tensor")
    core = lax.rem(me, CORES)
    chip = lax.div(me, CORES)
    partner = chip * CORES + (CORES - 1 - core)
    near_x = chip + 1 - 2 * lax.rem(chip, SIDE)
    near_y = chip + SIDE - 2 * SIDE * lax.div(chip, SIDE)
    first_chip = near_x + core * (near_y - near_x)
    other_chip = near_y + core * (near_x - near_y)
    far_chip = chips - 1 - chip

    def t_at(k):
        return lax.rem(t + k, n_t)

    barrier = pltpu.get_barrier_semaphore()
    for k in range(1, n_dp):
        pl.semaphore_signal(
            barrier, inc=1, device_id=(lax.rem(me + k, n_dp), t), device_id_type=MESH
        )
    for k in range(1, n_t):
        pl.semaphore_signal(barrier, inc=1, device_id=(me, t_at(k)), device_id_type=MESH)

    small = [
        pltpu.make_async_copy(source, target, local_sems.at[4 + i])
        for i, (source, target) in enumerate(
            (
                (pk_hbm, pk_buf),
                (len_hbm, len_buf),
                (gain_hbm.at[:, pl.ds(aligned(t, feat), feat)], gain),
                (tab_hbm, tab),
            )
        )
    ]
    load = pltpu.make_async_copy(roll_hbm, roll_in, local_sems.at[2])
    own_w = pltpu.make_async_copy(
        w_in.at[pl.ds(aligned(t, feat), feat)], wbuf.at[t], local_sems.at[0]
    )
    own_k = pltpu.make_async_copy(
        k_in.at[:, pl.ds(aligned(t, feat), feat)],
        kbuf.at[pl.ds(aligned(t, kd), kd)],
        local_sems.at[3],
    )
    own_o = pltpu.make_async_copy(
        o_in.at[:, pl.ds(aligned(t, feat), feat)], obuf.at[t], local_sems.at[1]
    )
    for copy in [*small, load, own_k, own_w, own_o]:
        copy.start()

    started, named = [], []

    def slot():
        named.append(recv_sems.at[len(named)])
        return named[-1]

    def send(source, target, device, arrival):
        copy = pltpu.make_async_remote_copy(
            src_ref=source,
            dst_ref=target,
            send_sem=send_sem,
            recv_sem=arrival,
            device_id=device,
            device_id_type=MESH,
        )
        copy.start()
        started.append(copy)

    def arrived(ref, arrival):
        pltpu.make_async_copy(ref, ref, arrival).wait()

    def w_at(u, h, c):
        return wbuf.at[u, pl.ds(aligned(h * CORES + c, w_sub), w_sub)]

    def k_at(u, h, c):
        return kbuf.at[
            pl.ds(aligned(u * chips + h, k_rows), k_rows), pl.ds(aligned(c, k_cols), k_cols)
        ]

    down = lax.broadcasted_iota(jnp.int32, (length, length), 0).astype(jnp.float32)
    across = lax.broadcasted_iota(jnp.int32, (length, length), 1).astype(jnp.float32)

    def part(value, size):
        return jnp.floor((value + 0.5) * (1.0 / size))

    def pick(mask, value, axis):
        return jnp.sum(jnp.where(mask, value, 0.0), axis=axis, keepdims=True)

    same = part(down, per_source) == part(across, per_source)
    diagonal = down == across
    for copy in small:
        copy.wait()
    len_all = len_buf[...].astype(jnp.float32)
    source_of = part(down[:, :1], per_source)
    table = jnp.zeros((length, per_source), jnp.float32)
    for i in range(n_dp):
        table = jnp.where(source_of == float(i), len_all[i : i + 1, :], table)
    within = down[:, :per_source] - source_of * per_source
    len_c = pick(across[:, :per_source] == within, table, 1)
    len_r = pick(diagonal, len_c, 0)
    pk_r = pk_buf[...].astype(jnp.float32)
    pk_c = pick(diagonal, pk_r, 1)
    src_start = pick(same & (across < down), len_r, 1)
    chosen = down == pk_r
    q_len_r = pick(chosen, len_c, 0)
    q_start_r = pick(chosen, src_start, 0)
    q_len_c = pick(across == pk_c, len_r, 1)
    earlier = same & (down < across)
    doc_start_r = pick(earlier, q_len_c, 0)
    q_src_r = part(pk_r, per_source)
    slot_r = pick(earlier & (part(pk_c, per_source) == q_src_r), 1.0, 0)
    mine = me.astype(jnp.float32)
    across_1 = across[:1]
    down_1 = down[:, :1]
    owner_r = part(across_1, per_source)
    target = jnp.where(q_src_r == mine, owner_r * (per_source // n_dp) + slot_r, -1.0)
    group = part(down_1, most)
    match = target == group
    token = down_1 - group * most
    row_sent = jnp.where(token < pick(match, q_len_r, 1), pick(match, q_start_r, 1) + token, -1.0)
    take_send = (across == row_sent).astype(jnp.float32).astype(jnp.bfloat16)

    tile = 256
    tiles = feat // tile
    load.wait()
    for i in range(tiles):
        at = slice(i * tile, (i + 1) * tile)
        sendb[:, at] = jnp.dot(
            take_send, roll_in[:, at], preferred_element_type=jnp.float32
        ).astype(jnp.bfloat16)

    pl.semaphore_wait(barrier, n_dp + n_t - 2)

    others = (1, 3, 2) if n_t == 4 else tuple(range(1, n_t))
    k_first = slot()
    for k in others:
        to = t_at(k)
        send(
            k_in.at[
                pl.ds(aligned(chip, k_rows), k_rows),
                pl.ds(aligned(to * CORES + core, k_cols), k_cols),
            ],
            k_at(t, chip, core),
            (me, to),
            k_first,
        )
    row_group = slot()

    def send_rows(to):
        send(
            sendb.at[pl.ds(aligned(to, block), block)],
            recvb.at[pl.ds(aligned(me, block), block)],
            (to, t),
            row_group,
        )

    for c in range(CORES):
        send_rows(far_chip * CORES + lax.rem(core + c, CORES))
    for c in range(CORES):
        send_rows(first_chip * CORES + lax.rem(core + c, CORES))
    send_rows(partner)
    w_first = {k: slot() for k in others}
    o_first = [slot() for _ in range(n_t)]

    def send_w(k):
        to = t_at(k)
        send(
            w_in.at[pl.ds(aligned(to * n_dp + me, w_sub), w_sub)], w_at(t, chip, core), (me, to),
            w_first[k],
        )

    send_w(1)

    o_parts = ((others[0], 0, 1), (others[1], 0, 1), (others[2], 0, 2), (others[2], 1, 2))

    def o_piece(p):
        _, index, split = o_parts[p]

        def at(u, h, c):
            size = o_sub // split
            return obuf.at[u, pl.ds(aligned((h * CORES + c) * split + index, size), size)]

        return at

    def send_o(p):
        j, index, split = o_parts[p]
        to, size = t_at(j), o_sub // split
        send(
            o_in.at[pl.ds(aligned(me * split + index, size), size), pl.ds(aligned(to, feat), feat)],
            o_piece(p)(t, chip, core),
            (me, to),
            o_first[p],
        )

    keep = pl.ds(aligned(me, block), block)
    recvb[keep, :] = sendb[keep, :]
    inside = (owner_r == mine) & (doc_start_r <= down) & (down < doc_start_r + q_len_r)
    is_valid = pick(inside, 1.0, 1)
    position = (down_1 - pick(inside, doc_start_r, 1)) * is_valid
    row_got = jnp.where(
        is_valid > 0.0, pick(inside, q_src_r * block + slot_r * most, 1) + position, -1.0
    )
    take_recv = (across == row_got).astype(jnp.float32).astype(jnp.bfloat16)
    pos = jnp.broadcast_to(position, (length, HD))
    pos_buf[...] = pos
    valid_buf[...] = jnp.broadcast_to(is_valid, (length, HD))
    cosine = jnp.zeros((length, HD), jnp.float32)
    sine = jnp.zeros((length, HD), jnp.float32)
    for m in range(most):
        at_m = pos == float(m)
        cosine = jnp.where(at_m, tab[m : m + 1, :], cosine)
        sine = jnp.where(at_m, tab[most + m : most + m + 1, :], sine)
    cos_buf[...] = cosine
    sin_buf[...] = sine
    mask_buf[...] = ((across <= down) & (across >= down - position)).astype(jnp.float32)
    fold_down = lax.broadcasted_iota(jnp.int32, (length, HD), 0)
    fold_across = lax.broadcasted_iota(jnp.int32, (length, HD), 1)
    fold_buf[...] = (
        (lax.rem(fold_down, most) == lax.rem(fold_across, most))
        .astype(jnp.float32)
        .astype(jnp.bfloat16)
    )

    first_dev = first_chip * CORES + core
    other_dev = other_chip * CORES + core

    def spread(at, j, hops):
        ref = at(t_at(n_t - j), chip, core)
        send(ref, ref, (first_dev, t), hops[0])
        send(ref, ref, (other_dev, t), hops[1])
        send(ref, ref, (partner, t), hops[2])

    def relay(at, j, hops):
        ref = at(t_at(n_t - j), first_chip, core)
        send(ref, ref, (other_dev, t), hops[1])
        send(ref, ref, (partner, t), hops[2])

    def settle(at, j, hops):
        for source in (other_chip, far_chip):
            ref = at(t_at(n_t - j), source, core)
            send(ref, ref, (partner, t), hops[2])

    k_hops = [slot() for _ in range(3)]
    w_hops = {j: [slot() for _ in range(3)] for j in others}
    o_hops = [[slot() for _ in range(3)] for _ in range(n_t)]

    def k_wait(count, arrival):
        arrived(
            kbuf.at[pl.ds(0, count * k_rows), pl.ds(0, k_cols)], arrival
        )

    def w_wait(count, j, arrival):
        arrived(wbuf.at[t_at(n_t - j), pl.ds(0, count * w_sub)], arrival)

    def o_wait(count, p, arrival):
        j, _, split = o_parts[p]
        arrived(obuf.at[t_at(n_t - j), pl.ds(0, count * o_sub // split)], arrival)

    def w_spread(j):
        w_wait(1, j, w_first[j])
        spread(w_at, j, w_hops[j])

    def w_relay(j):
        w_wait(1, j, w_hops[j][0])
        relay(w_at, j, w_hops[j])

    def w_settle(j):
        w_wait(2, j, w_hops[j][1])
        settle(w_at, j, w_hops[j])

    def o_spread(p):
        o_wait(1, p, o_first[p])
        spread(o_piece(p), o_parts[p][0], o_hops[p])

    def o_relay(p):
        o_wait(1, p, o_hops[p][0])
        relay(o_piece(p), o_parts[p][0], o_hops[p])

    def o_settle(p):
        o_wait(2, p, o_hops[p][1])
        settle(o_piece(p), o_parts[p][0], o_hops[p])

    one, three, two = others
    o_a, o_b, o_c, o_d = range(n_t)
    k_wait(n_t - 1, k_first)
    for j in others:
        spread(k_at, j, k_hops)
    for c in range(CORES):
        send_rows(other_chip * CORES + lax.rem(core + c, CORES))
    send_w(three)
    send_w(two)
    w_spread(one)
    send_o(o_a)
    k_wait(n_t - 1, k_hops[0])
    for j in others:
        relay(k_at, j, k_hops)
    arrived(recvb.at[pl.ds(0, (n_dp - 1) * block)], row_group)
    w_spread(three)
    squares = jnp.zeros((length, 1), jnp.float32)
    for i in range(tiles):
        at = slice(i * tile, (i + 1) * tile)
        x = jnp.dot(take_recv, recvb[:, at], preferred_element_type=jnp.float32)
        packed[:, at] = x.astype(jnp.bfloat16)
        scaled[:, at] = (x * gain[:, at]).astype(jnp.bfloat16)
        squares += jnp.sum(x * x, axis=1, keepdims=True)
    sq_part[...] = pick(diagonal, squares, 0)
    sq_group = slot()
    for k in others:
        send(sq_part, sq_recv.at[k - 1], (me, t_at(k)), sq_group)
    send_o(o_b)
    w_spread(two)
    w_relay(one)
    k_wait(2 * (n_t - 1), k_hops[1])
    for j in others:
        settle(k_at, j, k_hops)
    own_k.wait()
    k_wait(chips * (n_t - 1), k_hops[2])
    kv_groups = [slot() for _ in range(2)]

    def send_kv(c):
        cols = slice(c * HD, (c + 1) * HD)
        for k in others:
            to = t_at(k)
            send(
                kv_part.at[pl.ds(aligned(to, rows), rows), cols],
                kv_recv.at[k - 1, :, cols],
                (me, to),
                kv_groups[c],
            )

    for c in range(2):
        cols = slice(c * HD, (c + 1) * HD)
        kv_part[:, cols] = lax.dot_general(
            scaled[...], kbuf[cols, :], (((1,), (1,)), ((), ())),
            preferred_element_type=jnp.float32,
        ).astype(jnp.bfloat16)
        if c == 0:
            send_kv(0)
            send_o(o_c)
            send_o(o_d)
    w_relay(three)
    arrived(sq_recv, sq_group)
    sq = sq_part[...]
    for k in range(n_t - 1):
        sq += sq_recv[k]
    inverse = lax.rsqrt(sq / (feat * n_t) + epsilon)
    inv_buf[...] = jnp.broadcast_to(pick(diagonal, inverse, 1), (length, HD))

    def turn(v, c, s):
        return v * c + pltpu.roll(v, HD // 2, 1) * s

    def project(u):
        q = jnp.dot(scaled[...], wbuf[u], preferred_element_type=jnp.float32)
        for h in range(qd // HD):
            part_q = q[:, h * HD : (h + 1) * HD] * inv_buf[...]
            q_rot[:, pl.ds(aligned(u * (qd // HD) + h, HD), HD)] = turn(
                part_q, cos_buf[...], sin_buf[...]
            ).astype(jnp.bfloat16)

    own_w.wait()
    project(t)
    mine_rows = pl.ds(aligned(t, rows), rows)
    all_groups = [slot() for _ in range(2)]

    def share_kv(c):
        cols = slice(c * HD, (c + 1) * HD)
        arrived(kv_recv.at[:, :, cols], kv_groups[c])
        kv = kv_part[mine_rows, cols].astype(jnp.float32)
        for k in range(n_t - 1):
            kv += kv_recv[k, :, cols].astype(jnp.float32)
        kv = (kv * inv_buf[mine_rows, :]).astype(jnp.bfloat16)
        if c == 0:
            kv = turn(
                kv.astype(jnp.float32), cos_buf[mine_rows, :], sin_buf[mine_rows, :]
            ).astype(jnp.bfloat16)
        kv_all[mine_rows, cols] = kv
        at = kv_all.at[mine_rows, cols]
        for k in others:
            send(at, at, (me, t_at(k)), all_groups[c])

    w_relay(two)
    o_spread(o_a)
    w_settle(one)
    share_kv(0)
    send_kv(1)
    w_settle(three)
    o_spread(o_b)
    w_wait(chips, one, w_hops[one][2])
    project(t_at(n_t - one))
    w_settle(two)
    w_wait(chips, three, w_hops[three][2])
    project(t_at(n_t - three))
    o_relay(o_a)
    o_spread(o_c)
    w_wait(chips, two, w_hops[two][2])
    project(t_at(n_t - two))
    o_relay(o_b)
    o_spread(o_d)
    arrived(kv_all.at[pl.ds(0, (n_t - 1) * rows), pl.ds(0, HD)], all_groups[0])
    lane = lax.broadcasted_iota(jnp.int32, (half, HD), 1)
    line = lax.broadcasted_iota(jnp.int32, (half, HD), 0)
    cell = lax.div(lane, most)
    compact = jnp.zeros((half, HD), jnp.float32)
    for h in range(heads):
        scores = lax.dot_general(
            q_rot[:, h * HD : (h + 1) * HD], kv_all[:, :HD], (((1,), (1,)), ((), ())),
            preferred_element_type=jnp.float32,
        )
        scores = (scores * mask_buf[...]).astype(jnp.bfloat16)
        folded = jnp.dot(scores, fold_buf[...], preferred_element_type=jnp.float32)
        compact = jnp.where(cell == h, folded[:half], compact)
        compact = jnp.where(cell == heads + h, folded[half:], compact)
    score_part[...] = compact.astype(jnp.bfloat16)
    score_group = slot()
    for k in others:
        send(score_part, score_recv.at[k - 1], (me, t_at(k)), score_group)

    o_relay(o_c)
    share_kv(1)
    o_settle(o_a)
    o_relay(o_d)
    o_settle(o_b)
    o_settle(o_c)

    arrived(score_recv, score_group)
    total = score_part[...].astype(jnp.float32)
    for k in range(n_t - 1):
        total += score_recv[k].astype(jnp.float32)
    place = jnp.where(cell < heads, pos_buf[:half, :], pos_buf[half:, :])
    back = lax.rem(line - lane + HD, most).astype(jnp.float32)
    total = jnp.where(back <= place, total * (1.0 / math.sqrt(HD)), -jnp.inf)

    def around(value, combine):
        step = 1
        while step < most:
            low = lax.rem(lax.div(lane, step), 2) == 0
            value = combine(
                value,
                jnp.where(low, pltpu.roll(value, HD - step, 1), pltpu.roll(value, step, 1)),
            )
            step *= 2
        return value

    exponent = jnp.exp(total - around(total, jnp.maximum))
    weights = exponent / around(exponent, jnp.add)
    arrived(kv_all.at[pl.ds(0, (n_t - 1) * rows), pl.ds(HD, HD)], all_groups[1])
    for h in range(heads):
        chosen_w = jnp.concatenate(
            [jnp.where(cell == h, weights, 0.0), jnp.where(cell == heads + h, weights, 0.0)], axis=0
        ).astype(jnp.bfloat16)
        dense = lax.dot_general(
            chosen_w, fold_buf[...], (((1,), (1,)), ((), ())), preferred_element_type=jnp.float32
        )
        dense = (dense * mask_buf[...]).astype(jnp.bfloat16)
        ctx[:, h * HD : (h + 1) * HD] = jnp.dot(
            dense, kv_all[:, HD:], preferred_element_type=jnp.float32
        ).astype(jnp.bfloat16)

    o_settle(o_d)
    own_o.wait()
    for p in (o_a, o_b):
        o_wait(chips, p, o_hops[p][2])

    last = t_at(n_t - two)

    def take(u, at):
        return jnp.dot(
            ctx[:, pl.ds(aligned(u, o_rows), o_rows)], obuf[u, :, at],
            preferred_element_type=jnp.float32,
        )

    for i in range(tiles):
        at = slice(i * tile, (i + 1) * tile)
        result = packed[:, at].astype(jnp.float32)
        for u in (t, t_at(n_t - one), t_at(n_t - three)):
            result += take(u, at)
        acc[:, at] = result
    for p in (o_c, o_d):
        o_wait(chips, p, o_hops[p][2])
    for i in range(tiles):
        at = slice(i * tile, (i + 1) * tile)
        result = acc[:, at] + take(last, at)
        out[:, at] = jnp.where(valid_buf[:, :1] > 0.0, result, 0.0).astype(jnp.bfloat16)
    for copy in started:
        copy.wait_send()


def fused_body(rollout, lengths, packing, norm_gain, query_weight, keyval_weight, out_weight):
    n_dp, n_t = lax.axis_size("dp"), lax.axis_size("tensor")
    length, feat = rollout.shape
    per_source = lengths.shape[1]
    most = length // per_source
    qd, kd = query_weight.shape[1], keyval_weight.shape[1]
    frequency = np.float32(rope_base) ** (-np.arange(HD // 2, dtype=np.float32) * 2.0 / HD)
    angles = np.arange(most, dtype=np.float32)[:, None] * frequency[None, :].astype(np.float32)
    cos_tab = np.concatenate([np.cos(angles)] * 2, axis=1).astype(np.float32)
    sin_tab = np.concatenate([-np.sin(angles), np.sin(angles)], axis=1).astype(np.float32)
    rows = length // n_t
    groups = 4 + 4 * (n_t - 1) + 4 * n_t + 7
    vmem = pl.BlockSpec(memory_space=pltpu.VMEM)
    hbm = pl.BlockSpec(memory_space=pltpu.HBM)
    bf, f32 = jnp.bfloat16, jnp.float32
    return pl.pallas_call(
        functools.partial(fused_kernel, (n_dp, n_t, length, feat, per_source)),
        out_shape=jax.ShapeDtypeStruct((length, feat), bf),
        in_specs=[hbm] * 8,
        out_specs=vmem,
        scratch_shapes=[
            pltpu.VMEM((1, packing.shape[0]), jnp.int32),
            pltpu.VMEM(lengths.shape, jnp.int32),
            pltpu.VMEM((1, feat), f32),
            pltpu.VMEM((2 * most, HD), f32),
            pltpu.VMEM((n_t, feat, qd), bf),
            pltpu.VMEM((n_t * kd, feat), bf),
            pltpu.VMEM((n_t, out_weight.shape[0], feat), bf),
            pltpu.VMEM((length, feat), bf),
            pltpu.VMEM((length, feat), bf),
            pltpu.VMEM((length, feat), bf),
            pltpu.VMEM((length, feat), bf),
            pltpu.VMEM((length, feat), bf),
            pltpu.VMEM((length, n_t * qd), bf),
            pltpu.VMEM((length, 2 * HD), bf),
            pltpu.VMEM((n_t - 1, rows, 2 * HD), bf),
            pltpu.VMEM((length, 2 * HD), bf),
            pltpu.VMEM((length, n_t * qd), bf),
            pltpu.VMEM((length, HD), f32),
            pltpu.VMEM((length, HD), f32),
            pltpu.VMEM((length, HD), f32),
            pltpu.VMEM((length, HD), f32),
            pltpu.VMEM((length, HD), f32),
            pltpu.VMEM((length, length), f32),
            pltpu.VMEM((length, HD), bf),
            pltpu.VMEM((1, length), f32),
            pltpu.VMEM((n_t - 1, 1, length), f32),
            pltpu.VMEM((length // 2, HD), bf),
            pltpu.VMEM((n_t - 1, length // 2, HD), bf),
            pltpu.VMEM((length, feat), f32),
            pltpu.SemaphoreType.DMA,
            pltpu.SemaphoreType.DMA((groups,)),
            pltpu.SemaphoreType.DMA((8,)),
        ],
        compiler_params=pltpu.CompilerParams(
            collective_id=0, has_side_effects=True, vmem_limit_bytes=32 * 1024 * 1024
        ),
    )(
        *(
            pltpu.with_memory_space_constraint(operand, pltpu.HBM)
            for operand in (
                packing[None, :], lengths, norm_gain[None, :],
                jnp.asarray(np.concatenate([cos_tab, sin_tab])), rollout, query_weight,
                keyval_weight.T, out_weight,
            )
        )
    )


def body(rollout, lengths, packing, norm_gain, query_weight, keyval_weight, out_weight):
    n_dp, n_t = lax.axis_size("dp"), lax.axis_size("tensor")
    length, feat = rollout.shape
    per_source = lengths.shape[1]
    qd, kd = query_weight.shape[1], keyval_weight.shape[1]
    fits = (
        kd * n_t == 2 * HD
        and n_t == 4
        and n_dp == SIDE * SIDE * CORES
        and qd % HD == 0
        and n_t * qd // HD <= GROUP
        and per_source * 8 == length
        and n_t * qd // HD * 8 * 2 == HD
        and kd % (16 * n_dp // CORES) == 0
        and feat % (128 * CORES) == 0
        and length % (n_t * 16) == 0
        and length == 2 * HD
        and packing.shape[0] == length
        and (length // n_dp) % 16 == 0
        and feat % 512 == 0
        and per_source % n_dp == 0
    )
    chosen = fused_body if fits else plain_body
    return chosen(rollout, lengths, packing, norm_gain, query_weight, keyval_weight, out_weight)


def solution(mesh):
    in_specs = (
        P("dp", "tensor"),
        P(),
        P(),
        P(),
        P(None, "tensor"),
        P(None, "tensor"),
        P("tensor", None),
    )
    out_specs = P("dp", "tensor")
    return jax.shard_map(body, mesh=mesh, in_specs=in_specs, out_specs=out_specs, check_vma=False)
```

```python
import functools
import math

import numpy as np
import jax
import jax.numpy as jnp
from jax import lax
from jax.experimental import pallas as pl
from jax.experimental.pallas import tpu as pltpu
from jax.sharding import PartitionSpec as P

D = 6144
HD = 128
HQ_DEV = 2
GROUP = 8


epsilon = 1e-05
rope_base = 500000.0


def owner_map(lengths, packing, owner_id, pack_len):
    per_source = lengths.shape[1]
    chosen = lax.dynamic_slice_in_dim(packing, owner_id * per_source, per_source)
    ordered = jnp.take(lengths.reshape(-1), chosen)
    doc_start = jnp.cumsum(ordered) - ordered
    places = jnp.arange(pack_len, dtype=jnp.int32)
    inside = (places[:, None] >= doc_start[None, :]) & (
        places[:, None] < (doc_start + ordered)[None, :]
    )
    is_valid = jnp.any(inside, axis=1)
    slot_of = jnp.sum(
        jnp.where(inside, jnp.arange(per_source, dtype=jnp.int32)[None, :], 0), axis=1
    )
    response = jnp.take(chosen, slot_of)
    position = jnp.where(is_valid, places - jnp.take(doc_start, slot_of), 0)
    doc_id = jnp.where(is_valid, slot_of, per_source)
    return (response, position, doc_id, is_valid)


def rotate(values, position, head_dim):
    half_dim = head_dim // 2
    frequency = rope_base ** (-jnp.arange(half_dim, dtype=jnp.float32) * 2.0 / head_dim)
    angles = position.astype(jnp.float32)[:, None] * frequency[None, :]
    cosine = jnp.concatenate([jnp.cos(angles), jnp.cos(angles)], axis=1)[:, None, :]
    sine_table = jnp.concatenate([jnp.sin(angles), jnp.sin(angles)], axis=1)[:, None, :]
    turned = jnp.concatenate([-values[..., half_dim:], values[..., :half_dim]], axis=-1)
    return values * cosine + turned * sine_table


def plain_body(rollout, lengths, packing, norm_gain, query_weight, keyval_weight, out_weight):
    owner_id = lax.axis_index("dp")
    tensor_index = lax.axis_index("tensor")
    tensor_count = lax.axis_size("tensor")
    pack_len = rollout.shape[0]
    per_source = lengths.shape[1]
    response, position, doc_id, is_valid = owner_map(lengths, packing, owner_id, pack_len)
    source_start = jnp.cumsum(lengths, axis=1) - lengths
    global_row = (
        response // per_source * pack_len + jnp.take(source_start.reshape(-1), response) + position
    )
    portion = lax.all_gather(rollout, "dp", axis=0, tiled=True)
    within = is_valid & (global_row >= 0) & (global_row < portion.shape[0])
    picked = jnp.take(portion, jnp.clip(global_row, 0, portion.shape[0] - 1), axis=0)
    packed = jnp.where(within[:, None], picked, jnp.zeros_like(rollout))
    widened = lax.all_gather(packed, "tensor", axis=1, tiled=True).astype(jnp.float32)
    scaled = (widened * norm_gain[None, :]).astype(jnp.bfloat16)
    query_acc = jnp.dot(scaled, query_weight, preferred_element_type=jnp.float32)
    keyval_acc = jnp.dot(scaled, keyval_weight, preferred_element_type=jnp.float32)
    squares = jnp.sum(widened * widened, axis=1)
    query_acc, keyval_acc, squares = (query_acc, keyval_acc, squares)
    inverse = lax.rsqrt(squares / D + epsilon)
    queries = query_acc * inverse[:, None]
    keyval_share = (keyval_acc * inverse[:, None]).astype(jnp.bfloat16)
    keyval_all = lax.all_gather(keyval_share, "tensor", axis=1, tiled=True)
    kv_count = keyval_weight.shape[1] * tensor_count // (2 * HD)
    shared_head = tensor_index * HQ_DEV // GROUP
    keys = lax.dynamic_slice_in_dim(keyval_all, shared_head * HD, HD, 1)
    values = lax.dynamic_slice_in_dim(keyval_all, (kv_count + shared_head) * HD, HD, 1)
    q_rot = rotate(queries.reshape(pack_len, HQ_DEV, HD), position, HD).astype(jnp.bfloat16)
    k_rot = rotate(keys.astype(jnp.float32)[:, None, :], position, HD)[:, 0, :].astype(jnp.bfloat16)
    scores = jnp.einsum(
        "qhd,kd->hqk", q_rot, k_rot, preferred_element_type=jnp.float32
    ) / math.sqrt(HD)
    places = jnp.arange(pack_len, dtype=jnp.int32)
    allowed = (doc_id[:, None] == doc_id[None, :]) & (places[None, :] <= places[:, None])
    masked = jnp.where(allowed[None], scores, -jnp.inf)
    row_max = jnp.max(masked, axis=2, keepdims=True)
    exponent = jnp.exp(masked - row_max)
    weights = (exponent / jnp.sum(exponent, axis=2, keepdims=True)).astype(jnp.bfloat16)
    context = jnp.einsum("hqk,kd->qhd", weights, values, preferred_element_type=jnp.float32)
    context = context.astype(jnp.bfloat16).reshape(pack_len, HQ_DEV * HD)
    partial_sum = jnp.dot(context, out_weight, preferred_element_type=jnp.float32)
    summed = lax.psum_scatter(
        partial_sum.astype(jnp.bfloat16), "tensor", scatter_dimension=1, tiled=True
    ).astype(jnp.float32)
    result = jnp.where(is_valid[:, None], summed + packed.astype(jnp.float32), 0.0)
    return result.astype(jnp.bfloat16)


MESH = pl.DeviceIdType.MESH
CORES = 2
SIDE = 2


def aligned(index, size):
    return pl.multiple_of(index * size, size)


def fused_kernel(
    cfg, pk_hbm, len_hbm, gain_hbm, tab_hbm, roll_hbm, w_in, k_in, o_in, out,
    pk_buf, len_buf, gain, tab, wbuf, kbuf, obuf, roll_in, sendb, recvb, packed, scaled, q_rot, kv_part, kv_recv, kv_all, ctx,
    pos_buf, valid_buf, cos_buf, sin_buf, inv_buf, mask_buf, fold_buf, sq_part, sq_recv, score_part, score_recv, acc,
    send_sem, recv_sems, local_sems,
):
    n_dp, n_t, length, feat, per_source = cfg
    chips = n_dp // CORES
    w_sub = feat // n_dp
    kd = k_in.shape[0]
    k_rows, k_cols = kd // chips, feat // CORES
    o_rows = o_in.shape[0]
    o_sub = o_rows // n_dp
    block = length // n_dp
    most = length // per_source
    rows = length // n_t
    qd = w_in.shape[1]
    heads = n_t * qd // HD
    half = length // 2
    me = lax.axis_index("dp")
    t = lax.axis_index("tensor")
    core = lax.rem(me, CORES)
    chip = lax.div(me, CORES)
    partner = chip * CORES + (CORES - 1 - core)
    near_x = chip + 1 - 2 * lax.rem(chip, SIDE)
    near_y = chip + SIDE - 2 * SIDE * lax.div(chip, SIDE)
    first_chip = near_x + core * (near_y - near_x)
    other_chip = near_y + core * (near_x - near_y)
    far_chip = chips - 1 - chip

    def t_at(k):
        return lax.rem(t + k, n_t)

    barrier = pltpu.get_barrier_semaphore()
    for k in range(1, n_dp):
        pl.semaphore_signal(
            barrier, inc=1, device_id=(lax.rem(me + k, n_dp), t), device_id_type=MESH
        )
    for k in range(1, n_t):
        pl.semaphore_signal(barrier, inc=1, device_id=(me, t_at(k)), device_id_type=MESH)

    small = [
        pltpu.make_async_copy(source, target, local_sems.at[4 + i])
        for i, (source, target) in enumerate(
            (
                (pk_hbm, pk_buf),
                (len_hbm, len_buf),
                (gain_hbm.at[:, pl.ds(aligned(t, feat), feat)], gain),
                (tab_hbm, tab),
            )
        )
    ]
    load = pltpu.make_async_copy(roll_hbm, roll_in, local_sems.at[2])
    own_w = pltpu.make_async_copy(
        w_in.at[pl.ds(aligned(t, feat), feat)], wbuf.at[t], local_sems.at[0]
    )
    own_k = pltpu.make_async_copy(
        k_in.at[:, pl.ds(aligned(t, feat), feat)],
        kbuf.at[pl.ds(aligned(t, kd), kd)],
        local_sems.at[3],
    )
    own_o = pltpu.make_async_copy(
        o_in.at[:, pl.ds(aligned(t, feat), feat)], obuf.at[t], local_sems.at[1]
    )
    for copy in [*small, load, own_k, own_w, own_o]:
        copy.start()

    started, named = [], []

    def slot():
        named.append(recv_sems.at[len(named)])
        return named[-1]

    def send(source, target, device, arrival):
        copy = pltpu.make_async_remote_copy(
            src_ref=source,
            dst_ref=target,
            send_sem=send_sem,
            recv_sem=arrival,
            device_id=device,
            device_id_type=MESH,
        )
        copy.start()
        started.append(copy)

    def arrived(ref, arrival):
        pltpu.make_async_copy(ref, ref, arrival).wait()

    def w_at(u, h, c):
        return wbuf.at[u, pl.ds(aligned(h * CORES + c, w_sub), w_sub)]

    def k_at(u, h, c):
        return kbuf.at[
            pl.ds(aligned(u * chips + h, k_rows), k_rows), pl.ds(aligned(c, k_cols), k_cols)
        ]

    down = lax.broadcasted_iota(jnp.int32, (length, length), 0).astype(jnp.float32)
    across = lax.broadcasted_iota(jnp.int32, (length, length), 1).astype(jnp.float32)

    def part(value, size):
        return jnp.floor((value + 0.5) * (1.0 / size))

    def pick(mask, value, axis):
        return jnp.sum(jnp.where(mask, value, 0.0), axis=axis, keepdims=True)

    same = part(down, per_source) == part(across, per_source)
    diagonal = down == across
    for copy in small:
        copy.wait()
    len_all = len_buf[...].astype(jnp.float32)
    source_of = part(down[:, :1], per_source)
    table = jnp.zeros((length, per_source), jnp.float32)
    for i in range(n_dp):
        table = jnp.where(source_of == float(i), len_all[i : i + 1, :], table)
    within = down[:, :per_source] - source_of * per_source
    len_c = pick(across[:, :per_source] == within, table, 1)
    len_r = pick(diagonal, len_c, 0)
    pk_r = pk_buf[...].astype(jnp.float32)
    pk_c = pick(diagonal, pk_r, 1)
    src_start = pick(same & (across < down), len_r, 1)
    chosen = down == pk_r
    q_len_r = pick(chosen, len_c, 0)
    q_start_r = pick(chosen, src_start, 0)
    q_len_c = pick(across == pk_c, len_r, 1)
    earlier = same & (down < across)
    doc_start_r = pick(earlier, q_len_c, 0)
    q_src_r = part(pk_r, per_source)
    slot_r = pick(earlier & (part(pk_c, per_source) == q_src_r), 1.0, 0)
    mine = me.astype(jnp.float32)
    across_1 = across[:1]
    down_1 = down[:, :1]
    owner_r = part(across_1, per_source)
    target = jnp.where(q_src_r == mine, owner_r * (per_source // n_dp) + slot_r, -1.0)
    group = part(down_1, most)
    match = target == group
    token = down_1 - group * most
    row_sent = jnp.where(token < pick(match, q_len_r, 1), pick(match, q_start_r, 1) + token, -1.0)
    take_send = (across == row_sent).astype(jnp.float32).astype(jnp.bfloat16)

    tile = 256
    tiles = feat // tile
    load.wait()
    for i in range(tiles):
        at = slice(i * tile, (i + 1) * tile)
        sendb[:, at] = jnp.dot(
            take_send, roll_in[:, at], preferred_element_type=jnp.float32
        ).astype(jnp.bfloat16)

    pl.semaphore_wait(barrier, n_dp + n_t - 2)

    others = (1, 3, 2) if n_t == 4 else tuple(range(1, n_t))
    k_first = slot()
    for k in others:
        to = t_at(k)
        send(
            k_in.at[
                pl.ds(aligned(chip, k_rows), k_rows),
                pl.ds(aligned(to * CORES + core, k_cols), k_cols),
            ],
            k_at(t, chip, core),
            (me, to),
            k_first,
        )
    row_group = slot()

    def send_rows(to):
        send(
            sendb.at[pl.ds(aligned(to, block), block)],
            recvb.at[pl.ds(aligned(me, block), block)],
            (to, t),
            row_group,
        )

    for c in range(CORES):
        send_rows(far_chip * CORES + lax.rem(core + c, CORES))
    for c in range(CORES):
        send_rows(first_chip * CORES + lax.rem(core + c, CORES))
    send_rows(partner)
    w_first = {k: slot() for k in others}
    o_first = [slot() for _ in range(n_t)]

    def send_w(k):
        to = t_at(k)
        send(
            w_in.at[pl.ds(aligned(to * n_dp + me, w_sub), w_sub)], w_at(t, chip, core), (me, to),
            w_first[k],
        )

    send_w(1)
    send_w(others[1])

    o_parts = ((others[0], 0, 1), (others[1], 0, 1), (others[2], 0, 2), (others[2], 1, 2))

    def o_piece(p):
        _, index, split = o_parts[p]

        def at(u, h, c):
            size = o_sub // split
            return obuf.at[u, pl.ds(aligned((h * CORES + c) * split + index, size), size)]

        return at

    def send_o(p):
        j, index, split = o_parts[p]
        to, size = t_at(j), o_sub // split
        send(
            o_in.at[pl.ds(aligned(me * split + index, size), size), pl.ds(aligned(to, feat), feat)],
            o_piece(p)(t, chip, core),
            (me, to),
            o_first[p],
        )

    keep = pl.ds(aligned(me, block), block)
    recvb[keep, :] = sendb[keep, :]
    inside = (owner_r == mine) & (doc_start_r <= down) & (down < doc_start_r + q_len_r)
    is_valid = pick(inside, 1.0, 1)
    position = (down_1 - pick(inside, doc_start_r, 1)) * is_valid
    row_got = jnp.where(
        is_valid > 0.0, pick(inside, q_src_r * block + slot_r * most, 1) + position, -1.0
    )
    take_recv = (across == row_got).astype(jnp.float32).astype(jnp.bfloat16)
    pos = jnp.broadcast_to(position, (length, HD))
    pos_buf[...] = pos
    valid_buf[...] = jnp.broadcast_to(is_valid, (length, HD))
    cosine = jnp.zeros((length, HD), jnp.float32)
    sine = jnp.zeros((length, HD), jnp.float32)
    for m in range(most):
        at_m = pos == float(m)
        cosine = jnp.where(at_m, tab[m : m + 1, :], cosine)
        sine = jnp.where(at_m, tab[most + m : most + m + 1, :], sine)
    cos_buf[...] = cosine
    sin_buf[...] = sine
    mask_buf[...] = ((across <= down) & (across >= down - position)).astype(jnp.float32)
    fold_down = lax.broadcasted_iota(jnp.int32, (length, HD), 0)
    fold_across = lax.broadcasted_iota(jnp.int32, (length, HD), 1)
    fold_buf[...] = (
        (lax.rem(fold_down, most) == lax.rem(fold_across, most))
        .astype(jnp.float32)
        .astype(jnp.bfloat16)
    )

    first_dev = first_chip * CORES + core
    other_dev = other_chip * CORES + core

    def spread(at, j, hops):
        ref = at(t_at(n_t - j), chip, core)
        send(ref, ref, (first_dev, t), hops[0])
        send(ref, ref, (other_dev, t), hops[1])
        send(ref, ref, (partner, t), hops[2])

    def relay(at, j, hops):
        ref = at(t_at(n_t - j), first_chip, core)
        send(ref, ref, (other_dev, t), hops[1])
        send(ref, ref, (partner, t), hops[2])

    def settle(at, j, hops):
        for source in (other_chip, far_chip):
            ref = at(t_at(n_t - j), source, core)
            send(ref, ref, (partner, t), hops[2])

    k_hops = [slot() for _ in range(3)]
    w_hops = {j: [slot() for _ in range(3)] for j in others}
    o_hops = [[slot() for _ in range(3)] for _ in range(n_t)]

    def k_wait(count, arrival):
        arrived(
            kbuf.at[pl.ds(0, count * k_rows), pl.ds(0, k_cols)], arrival
        )

    def w_wait(count, j, arrival):
        arrived(wbuf.at[t_at(n_t - j), pl.ds(0, count * w_sub)], arrival)

    def o_wait(count, p, arrival):
        j, _, split = o_parts[p]
        arrived(obuf.at[t_at(n_t - j), pl.ds(0, count * o_sub // split)], arrival)

    def w_spread(j):
        w_wait(1, j, w_first[j])
        spread(w_at, j, w_hops[j])

    def w_relay(j):
        w_wait(1, j, w_hops[j][0])
        relay(w_at, j, w_hops[j])

    def w_settle(j):
        w_wait(2, j, w_hops[j][1])
        settle(w_at, j, w_hops[j])

    def o_spread(p):
        o_wait(1, p, o_first[p])
        spread(o_piece(p), o_parts[p][0], o_hops[p])

    def o_relay(p):
        o_wait(1, p, o_hops[p][0])
        relay(o_piece(p), o_parts[p][0], o_hops[p])

    def o_settle(p):
        o_wait(2, p, o_hops[p][1])
        settle(o_piece(p), o_parts[p][0], o_hops[p])

    one, three, two = others
    o_a, o_b, o_c, o_d = range(n_t)
    k_wait(n_t - 1, k_first)
    for j in others:
        spread(k_at, j, k_hops)
    for c in range(CORES):
        send_rows(other_chip * CORES + lax.rem(core + c, CORES))
    send_w(two)
    w_spread(one)
    send_o(o_a)
    k_wait(n_t - 1, k_hops[0])
    for j in others:
        relay(k_at, j, k_hops)
    arrived(recvb.at[pl.ds(0, (n_dp - 1) * block)], row_group)
    w_spread(three)
    squares = jnp.zeros((length, 1), jnp.float32)
    for i in range(tiles):
        at = slice(i * tile, (i + 1) * tile)
        x = jnp.dot(take_recv, recvb[:, at], preferred_element_type=jnp.float32)
        packed[:, at] = x.astype(jnp.bfloat16)
        scaled[:, at] = (x * gain[:, at]).astype(jnp.bfloat16)
        squares += jnp.sum(x * x, axis=1, keepdims=True)
    sq_part[...] = pick(diagonal, squares, 0)
    sq_group = slot()
    for k in others:
        send(sq_part, sq_recv.at[k - 1], (me, t_at(k)), sq_group)
    send_o(o_b)
    w_spread(two)
    w_relay(one)
    k_wait(2 * (n_t - 1), k_hops[1])
    for j in others:
        settle(k_at, j, k_hops)
    own_k.wait()
    k_wait(chips * (n_t - 1), k_hops[2])
    kv_groups = [slot() for _ in range(2)]

    def send_kv(c):
        cols = slice(c * HD, (c + 1) * HD)
        for k in others:
            to = t_at(k)
            send(
                kv_part.at[pl.ds(aligned(to, rows), rows), cols],
                kv_recv.at[k - 1, :, cols],
                (me, to),
                kv_groups[c],
            )

    for c in range(2):
        cols = slice(c * HD, (c + 1) * HD)
        kv_part[:, cols] = lax.dot_general(
            scaled[...], kbuf[cols, :], (((1,), (1,)), ((), ())),
            preferred_element_type=jnp.float32,
        ).astype(jnp.bfloat16)
        if c == 0:
            send_kv(0)
            send_o(o_c)
            send_o(o_d)
    w_relay(three)
    arrived(sq_recv, sq_group)
    sq = sq_part[...]
    for k in range(n_t - 1):
        sq += sq_recv[k]
    inverse = lax.rsqrt(sq / (feat * n_t) + epsilon)
    inv_buf[...] = jnp.broadcast_to(pick(diagonal, inverse, 1), (length, HD))

    def turn(v, c, s):
        return v * c + pltpu.roll(v, HD // 2, 1) * s

    def project(u):
        q = jnp.dot(scaled[...], wbuf[u], preferred_element_type=jnp.float32)
        for h in range(qd // HD):
            part_q = q[:, h * HD : (h + 1) * HD] * inv_buf[...]
            q_rot[:, pl.ds(aligned(u * (qd // HD) + h, HD), HD)] = turn(
                part_q, cos_buf[...], sin_buf[...]
            ).astype(jnp.bfloat16)

    own_w.wait()
    project(t)
    mine_rows = pl.ds(aligned(t, rows), rows)
    all_groups = [slot() for _ in range(2)]

    def share_kv(c):
        cols = slice(c * HD, (c + 1) * HD)
        arrived(kv_recv.at[:, :, cols], kv_groups[c])
        kv = kv_part[mine_rows, cols].astype(jnp.float32)
        for k in range(n_t - 1):
            kv += kv_recv[k, :, cols].astype(jnp.float32)
        kv = (kv * inv_buf[mine_rows, :]).astype(jnp.bfloat16)
        if c == 0:
            kv = turn(
                kv.astype(jnp.float32), cos_buf[mine_rows, :], sin_buf[mine_rows, :]
            ).astype(jnp.bfloat16)
        kv_all[mine_rows, cols] = kv
        at = kv_all.at[mine_rows, cols]
        for k in others:
            send(at, at, (me, t_at(k)), all_groups[c])

    w_relay(two)
    o_spread(o_a)
    w_settle(one)
    share_kv(0)
    send_kv(1)
    w_settle(three)
    o_spread(o_b)
    w_wait(chips, one, w_hops[one][2])
    project(t_at(n_t - one))
    w_settle(two)
    w_wait(chips, three, w_hops[three][2])
    project(t_at(n_t - three))
    o_relay(o_a)
    o_spread(o_c)
    w_wait(chips, two, w_hops[two][2])
    project(t_at(n_t - two))
    o_relay(o_b)
    o_spread(o_d)
    arrived(kv_all.at[pl.ds(0, (n_t - 1) * rows), pl.ds(0, HD)], all_groups[0])
    lane = lax.broadcasted_iota(jnp.int32, (half, HD), 1)
    line = lax.broadcasted_iota(jnp.int32, (half, HD), 0)
    cell = lax.div(lane, most)
    compact = jnp.zeros((half, HD), jnp.float32)
    for h in range(heads):
        scores = lax.dot_general(
            q_rot[:, h * HD : (h + 1) * HD], kv_all[:, :HD], (((1,), (1,)), ((), ())),
            preferred_element_type=jnp.float32,
        )
        scores = (scores * mask_buf[...]).astype(jnp.bfloat16)
        folded = jnp.dot(scores, fold_buf[...], preferred_element_type=jnp.float32)
        compact = jnp.where(cell == h, folded[:half], compact)
        compact = jnp.where(cell == heads + h, folded[half:], compact)
    score_part[...] = compact.astype(jnp.bfloat16)
    score_group = slot()
    for k in others:
        send(score_part, score_recv.at[k - 1], (me, t_at(k)), score_group)

    o_relay(o_c)
    share_kv(1)
    o_settle(o_a)
    o_relay(o_d)
    o_settle(o_b)
    o_settle(o_c)

    arrived(score_recv, score_group)
    total = score_part[...].astype(jnp.float32)
    for k in range(n_t - 1):
        total += score_recv[k].astype(jnp.float32)
    place = jnp.where(cell < heads, pos_buf[:half, :], pos_buf[half:, :])
    back = lax.rem(line - lane + HD, most).astype(jnp.float32)
    total = jnp.where(back <= place, total * (1.0 / math.sqrt(HD)), -jnp.inf)

    def around(value, combine):
        step = 1
        while step < most:
            low = lax.rem(lax.div(lane, step), 2) == 0
            value = combine(
                value,
                jnp.where(low, pltpu.roll(value, HD - step, 1), pltpu.roll(value, step, 1)),
            )
            step *= 2
        return value

    exponent = jnp.exp(total - around(total, jnp.maximum))
    weights = exponent / around(exponent, jnp.add)
    arrived(kv_all.at[pl.ds(0, (n_t - 1) * rows), pl.ds(HD, HD)], all_groups[1])
    for h in range(heads):
        chosen_w = jnp.concatenate(
            [jnp.where(cell == h, weights, 0.0), jnp.where(cell == heads + h, weights, 0.0)], axis=0
        ).astype(jnp.bfloat16)
        dense = lax.dot_general(
            chosen_w, fold_buf[...], (((1,), (1,)), ((), ())), preferred_element_type=jnp.float32
        )
        dense = (dense * mask_buf[...]).astype(jnp.bfloat16)
        ctx[:, h * HD : (h + 1) * HD] = jnp.dot(
            dense, kv_all[:, HD:], preferred_element_type=jnp.float32
        ).astype(jnp.bfloat16)

    o_settle(o_d)
    own_o.wait()
    for p in (o_a, o_b):
        o_wait(chips, p, o_hops[p][2])

    last = t_at(n_t - two)

    def take(u, at):
        return jnp.dot(
            ctx[:, pl.ds(aligned(u, o_rows), o_rows)], obuf[u, :, at],
            preferred_element_type=jnp.float32,
        )

    for i in range(tiles):
        at = slice(i * tile, (i + 1) * tile)
        result = packed[:, at].astype(jnp.float32)
        for u in (t, t_at(n_t - one), t_at(n_t - three)):
            result += take(u, at)
        acc[:, at] = result
    for p in (o_c, o_d):
        o_wait(chips, p, o_hops[p][2])
    for i in range(tiles):
        at = slice(i * tile, (i + 1) * tile)
        result = acc[:, at] + take(last, at)
        out[:, at] = jnp.where(valid_buf[:, :1] > 0.0, result, 0.0).astype(jnp.bfloat16)
    for copy in started:
        copy.wait_send()


def fused_body(rollout, lengths, packing, norm_gain, query_weight, keyval_weight, out_weight):
    n_dp, n_t = lax.axis_size("dp"), lax.axis_size("tensor")
    length, feat = rollout.shape
    per_source = lengths.shape[1]
    most = length // per_source
    qd, kd = query_weight.shape[1], keyval_weight.shape[1]
    frequency = np.float32(rope_base) ** (-np.arange(HD // 2, dtype=np.float32) * 2.0 / HD)
    angles = np.arange(most, dtype=np.float32)[:, None] * frequency[None, :].astype(np.float32)
    cos_tab = np.concatenate([np.cos(angles)] * 2, axis=1).astype(np.float32)
    sin_tab = np.concatenate([-np.sin(angles), np.sin(angles)], axis=1).astype(np.float32)
    rows = length // n_t
    groups = 4 + 4 * (n_t - 1) + 4 * n_t + 7
    vmem = pl.BlockSpec(memory_space=pltpu.VMEM)
    hbm = pl.BlockSpec(memory_space=pltpu.HBM)
    bf, f32 = jnp.bfloat16, jnp.float32
    return pl.pallas_call(
        functools.partial(fused_kernel, (n_dp, n_t, length, feat, per_source)),
        out_shape=jax.ShapeDtypeStruct((length, feat), bf),
        in_specs=[hbm] * 8,
        out_specs=vmem,
        scratch_shapes=[
            pltpu.VMEM((1, packing.shape[0]), jnp.int32),
            pltpu.VMEM(lengths.shape, jnp.int32),
            pltpu.VMEM((1, feat), f32),
            pltpu.VMEM((2 * most, HD), f32),
            pltpu.VMEM((n_t, feat, qd), bf),
            pltpu.VMEM((n_t * kd, feat), bf),
            pltpu.VMEM((n_t, out_weight.shape[0], feat), bf),
            pltpu.VMEM((length, feat), bf),
            pltpu.VMEM((length, feat), bf),
            pltpu.VMEM((length, feat), bf),
            pltpu.VMEM((length, feat), bf),
            pltpu.VMEM((length, feat), bf),
            pltpu.VMEM((length, n_t * qd), bf),
            pltpu.VMEM((length, 2 * HD), bf),
            pltpu.VMEM((n_t - 1, rows, 2 * HD), bf),
            pltpu.VMEM((length, 2 * HD), bf),
            pltpu.VMEM((length, n_t * qd), bf),
            pltpu.VMEM((length, HD), f32),
            pltpu.VMEM((length, HD), f32),
            pltpu.VMEM((length, HD), f32),
            pltpu.VMEM((length, HD), f32),
            pltpu.VMEM((length, HD), f32),
            pltpu.VMEM((length, length), f32),
            pltpu.VMEM((length, HD), bf),
            pltpu.VMEM((1, length), f32),
            pltpu.VMEM((n_t - 1, 1, length), f32),
            pltpu.VMEM((length // 2, HD), bf),
            pltpu.VMEM((n_t - 1, length // 2, HD), bf),
            pltpu.VMEM((length, feat), f32),
            pltpu.SemaphoreType.DMA,
            pltpu.SemaphoreType.DMA((groups,)),
            pltpu.SemaphoreType.DMA((8,)),
        ],
        compiler_params=pltpu.CompilerParams(
            collective_id=0, has_side_effects=True, vmem_limit_bytes=32 * 1024 * 1024
        ),
    )(
        *(
            pltpu.with_memory_space_constraint(operand, pltpu.HBM)
            for operand in (
                packing[None, :], lengths, norm_gain[None, :],
                jnp.asarray(np.concatenate([cos_tab, sin_tab])), rollout, query_weight,
                keyval_weight.T, out_weight,
            )
        )
    )


def body(rollout, lengths, packing, norm_gain, query_weight, keyval_weight, out_weight):
    n_dp, n_t = lax.axis_size("dp"), lax.axis_size("tensor")
    length, feat = rollout.shape
    per_source = lengths.shape[1]
    qd, kd = query_weight.shape[1], keyval_weight.shape[1]
    fits = (
        kd * n_t == 2 * HD
        and n_t == 4
        and n_dp == SIDE * SIDE * CORES
        and qd % HD == 0
        and n_t * qd // HD <= GROUP
        and per_source * 8 == length
        and n_t * qd // HD * 8 * 2 == HD
        and kd % (16 * n_dp // CORES) == 0
        and feat % (128 * CORES) == 0
        and length % (n_t * 16) == 0
        and length == 2 * HD
        and packing.shape[0] == length
        and (length // n_dp) % 16 == 0
        and feat % 512 == 0
        and per_source % n_dp == 0
    )
    chosen = fused_body if fits else plain_body
    return chosen(rollout, lengths, packing, norm_gain, query_weight, keyval_weight, out_weight)


def solution(mesh):
    in_specs = (
        P("dp", "tensor"),
        P(),
        P(),
        P(),
        P(None, "tensor"),
        P(None, "tensor"),
        P("tensor", None),
    )
    out_specs = P("dp", "tensor")
    return jax.shard_map(body, mesh=mesh, in_specs=in_specs, out_specs=out_specs, check_vma=False)
```
